128 devices in a mesh: rep: 1, dp: 128 (over x, y, z, core).
Axes of the slice: x: 4, y: 4, z: 4, core: 2. Of those that a mesh axis runs over, the one named last changes fastest.
Arguments:
- g_w_gate: bfloat16 [128, 2, 768, 1792], P(('rep', 'dp'))
- g_w_up: bfloat16 [128, 2, 768, 1792], P(('rep', 'dp'))
- g_w_down: bfloat16 [128, 2, 1792, 768], P(('rep', 'dp'))
- w_gate: bfloat16 [2, 768, 1792], replicated
- w_up: bfloat16 [2, 768, 1792], replicated
- w_down: bfloat16 [2, 1792, 768], replicated
- m_w_gate: float32 [2, 768, 1792], P(None, 'dp')
- m_w_up: float32 [2, 768, 1792], P(None, 'dp')
- m_w_down: float32 [2, 1792, 768], P(None, 'dp')
- v_w_gate: float32 [2, 768, 1792], P(None, 'dp')
- v_w_up: float32 [2, 768, 1792], P(None, 'dp')
- v_w_down: float32 [2, 1792, 768], P(None, 'dp')
Outputs:
- output 1: bfloat16 [2, 768, 1792], P('rep')
- output 2: bfloat16 [2, 768, 1792], P('rep')
- output 3: bfloat16 [2, 1792, 768], P('rep')
- output 4: float32 [2, 768, 1792], P('rep', 'dp')
- output 5: float32 [2, 768, 1792], P('rep', 'dp')
- output 6: float32 [2, 1792, 768], P('rep', 'dp')
- output 7: float32 [2, 768, 1792], P('rep', 'dp')
- output 8: float32 [2, 768, 1792], P('rep', 'dp')
- output 9: float32 [2, 1792, 768], P('rep', 'dp')
All inputs are finite; a program needn't handle non-finite values.
Results may differ from the reference program's by a relative error of at most 0.022.
Values are sent between devices in bfloat16 or wider.
A program may use at most 1.5 GiB of HBM per device.

```python
import jax
import jax.numpy as jnp
from jax import lax

DEVICES = 128
D = 768
FF = 1792
LAYERS = 2
NAMES = ("w_gate", "w_up", "w_down")
SHAPES = {"w_gate": (LAYERS, D, FF), "w_up": (LAYERS, D, FF), "w_down": (LAYERS, FF, D)}


def setup_inputs(seed: int = 0, part: int = 0) -> dict:
    kz, *keys = jax.random.split(jax.random.key(seed), 1 + 5 * len(NAMES))
    loud = 2.0 ** jax.random.uniform(kz, (), jnp.float32, -1.0, 1.0)
    drawn = {}
    for name, key, both in zip(NAMES, keys[:3], keys[3:6], strict=True):
        own = jax.random.normal(jax.random.fold_in(key, part), (DEVICES, *SHAPES[name]), jnp.float32)
        shared = jax.random.normal(jax.random.fold_in(both, part), SHAPES[name], jnp.float32)
        drawn["g_" + name] = (loud * (0.7 * shared / DEVICES + 0.7 * own * DEVICES**-0.5)).astype(jnp.bfloat16)
    for name, key in zip(NAMES, keys[6:9], strict=True):
        drawn[name] = (jax.random.normal(key, SHAPES[name], jnp.float32) * SHAPES[name][1] ** -0.5).astype(jnp.bfloat16)
    for name, key in zip(NAMES, keys[9:12], strict=True):
        drawn["m_" + name] = loud * 0.5 * jax.random.normal(key, SHAPES[name], jnp.float32)
    for name, key in zip(NAMES, keys[12:15], strict=True):
        drawn["v_" + name] = loud * loud * jax.random.uniform(key, SHAPES[name], jnp.float32, 0.5, 1.5)
    return drawn


def adamw(w, m, v, g):
    m = 0.9 * m + 0.1 * g
    v = 0.95 * v + 0.05 * g * g
    step = m * lax.rsqrt(v + 1e-8) + 0.1 * w
    return (w - 0.02 * step).astype(jnp.bfloat16), m, v


def reference(g_w_gate, g_w_up, g_w_down, w_gate, w_up, w_down, m_w_gate, m_w_up, m_w_down, v_w_gate, v_w_up, v_w_down):
    def total(terms):
        return lax.scan(lambda so_far, term: (so_far + term.astype(jnp.float32), None), jnp.zeros(terms.shape[1:], jnp.float32), terms)[0]

    gradients = [total(terms).astype(jnp.bfloat16).astype(jnp.float32) for terms in (g_w_gate, g_w_up, g_w_down)]
    new = [
        adamw(w.astype(jnp.float32), m, v, g)
        for w, m, v, g in zip((w_gate, w_up, w_down), (m_w_gate, m_w_up, m_w_down), (v_w_gate, v_w_up, v_w_down), gradients, strict=True)
    ]
    return tuple(one[which] for which in range(3) for one in new)
```

```python
import jax
import jax.numpy as jnp
from jax import lax
from jax.experimental import pallas as pl
from jax.experimental.pallas import tpu as pltpu
from jax.sharding import PartitionSpec as P

MESH = pl.DeviceIdType.MESH
BF, F32 = jnp.bfloat16, jnp.float32

COLS = (1792, 1792, 768)
R = (48, 48, 112)
RC = (12, 12, 28)
RP = (16, 16, 32)
H = (6, 6, 14)
AXES = ((0, 1, 2), (1, 2, 0), (2, 0, 1))
TILES = ((2, 2, 3), (2, 2, 3), (1, 1, 1))
CHUNKS = len(TILES[0])
MSGS = 25
WHEN = (0, 4, 8, 12, 15, 18, 20, 22, 24, 26, 28, 31, 34, 37, 42, 47, 55)
LAG = 8


def adamw(w, m, v, g):
    m = 0.9 * m + 0.1 * g
    v = 0.95 * v + 0.05 * g * g
    step = m * lax.rsqrt(v + 1e-8) + 0.1 * w
    return (w - 0.02 * step).astype(BF), m, v


class Unit:
    def __init__(self, color, chunk, way, c0, cn, uid):
        self.a, self.chunk, self.s, self.c0, self.cn, self.u = color, chunk, way, c0, cn, uid
        self.cols = pl.ds(c0, cn)


def units():
    found, uid = [], 0
    for a in range(3):
        c0 = 0
        for k, t in enumerate(TILES[a]):
            for way in (1, -1):
                found.append(Unit(a, k, way, c0, 128 * t, uid))
                c0 += 128 * t
                uid += 1
        assert c0 == COLS[a]
    return found


def comm_kernel(*refs):
    it = iter(refs)

    def take(n):
        return [next(it) for _ in range(n)]

    g, w, m, v = take(3), take(3), take(3), take(3)
    out, gfin = take(3), take(3)
    own, part = take(3), take(3)
    psum = next(it)
    s1, r1, a1, s2, r2, a2, s3, r3 = (take(3) for _ in range(8))
    gs, gr, wx, ws, ag3 = (take(3) for _ in range(5))
    ag2u, tmp, osem, ssem, rsem = take(5)
    all_units = units()

    me = lax.axis_index("dp")
    rep = lax.axis_index("rep")
    c = lax.rem(me, 2)
    pos = (me // 32, lax.rem(me // 8, 4), lax.rem(me // 2, 4))
    strides = (32, 8, 2)
    partner = me + 1 - 2 * c

    def near(axis, d):
        return me + (lax.rem(pos[axis] + d + 4, 4) - pos[axis]) * strides[axis]

    def send(u, i, src, dst, to):
        pltpu.make_async_remote_copy(
            src_ref=src, dst_ref=dst, send_sem=ssem.at[u.u, i], recv_sem=rsem.at[u.u, i], device_id=(rep, to), device_id_type=MESH
        ).start()

    def waiter(u, i, ref):
        return pltpu.make_async_remote_copy(
            src_ref=ref, dst_ref=ref, send_sem=ssem.at[u.u, i], recv_sem=rsem.at[u.u, i], device_id=(rep, partner), device_id_type=MESH
        )

    pending = []

    def post(u, i, src, dst, to):
        send(u, i, src, dst, to)
        pending.append((u, i, src))

    def got(u, i, ref):
        waiter(u, i, ref).wait_recv()

    def loads(u):
        return pltpu.make_async_copy(g[u.a].at[c, :, :, :, u.cols], own[u.a].at[:, :, :, u.cols], osem.at[u.u])

    def mine1(u, q, i):
        if u.a == 2:
            return psum[q, i, :, u.cols]
        at = (q, i) if u.a == 0 else (i, q)
        return own[u.a][(*at, slice(None), u.cols)].astype(F32) + part[u.a][(*at, slice(None), u.cols)].astype(F32)

    def axis(u, phase):
        return AXES[u.a][phase]

    def at(u, phase, d):
        return lax.rem(pos[axis(u, phase)] + d + 4, 4)

    S = slice(None)

    def sum1(u, i, q, came):
        @pl.loop(0, 4)
        def _(j):
            x = mine1(u, q, j)
            if came:
                x = x + r1[u.a][0, j, :, u.cols].astype(F32)
            s1[u.a][i, j, :, u.cols] = x.astype(BF)

        post(u, i, s1[u.a].at[i, :, :, u.cols], r1[u.a].at[i, :, :, u.cols], near(axis(u, 0), -u.s if i == 1 else u.s))

    def sum2(u, i, q, came):
        x = a1[u.a][q, :, u.cols]
        if came:
            x = x + r2[u.a][0, :, u.cols].astype(F32)
        s2[u.a][i, :, u.cols] = x.astype(BF)
        post(u, 3 + i, s2[u.a].at[i, :, u.cols], r2[u.a].at[i, :, u.cols], near(axis(u, 1), -u.s if i == 1 else u.s))

    def sum3(u, i, q, came):
        x = a2[u.a][q, :, u.cols]
        if came:
            x = x + r3[u.a][0, :, u.cols].astype(F32)
        s3[u.a][i, :, u.cols] = x.astype(BF)
        post(u, 6 + i, s3[u.a].at[i, :, u.cols], r3[u.a].at[i, :, u.cols], near(axis(u, 2), -u.s if i == 1 else u.s))

    def start_sum(u, phase, fn):
        fn(u, 0, at(u, phase, 2), False)
        fn(u, 1, at(u, phase, -u.s), False)

    def each(k):
        return [u for u in all_units if u.chunk == k]

    def st0(k):
        for u in each(k):
            post(u, 20, g[u.a].at[1 - c, :, :, :, u.cols], part[u.a].at[:, :, :, u.cols], partner)

    def st1(k):
        for u in each(k):
            loads(u).wait()
            got(u, 20, part[u.a].at[:, :, :, u.cols])
            if u.a == 2:

                @pl.loop(0, 4)
                def _(x):
                    for y in range(4):
                        t = own[2][x, y, :, u.cols].astype(F32) + part[2][x, y, :, u.cols].astype(F32)
                        for z in range(4):
                            psum[z, x, 28 * y : 28 * y + 28, u.cols] = t[28 * z : 28 * z + 28]

            sum1(u, 0, at(u, 0, 2), False)
        for u in each(k):
            sum1(u, 1, at(u, 0, -u.s), False)

    def st2(k):
        for u in each(k):
            got(u, 0, r1[u.a].at[0, :, :, u.cols])
            sum1(u, 2, at(u, 0, u.s), True)

    def st3(k):
        for u in each(k):
            got(u, 1, r1[u.a].at[1, :, :, u.cols])
            got(u, 2, r1[u.a].at[2, :, :, u.cols])
            q = pos[axis(u, 0)]

            def total(j):
                return mine1(u, q, j) + r1[u.a][1, j, :, u.cols].astype(F32) + r1[u.a][2, j, :, u.cols].astype(F32)

            if u.a == 1:
                for j in range(4):
                    t = total(j)
                    for z in range(4):
                        a1[1][z, 12 * j : 12 * j + 12, u.cols] = t[12 * z : 12 * z + 12]
            else:

                @pl.loop(0, 4)
                def _(j):
                    a1[u.a][j, :, u.cols] = total(j)

            sum2(u, 0, at(u, 1, 2), False)
        for u in each(k):
            sum2(u, 1, at(u, 1, -u.s), False)

    def st4(k):
        for u in each(k):
            got(u, 3, r2[u.a].at[0, :, u.cols])
            sum2(u, 2, at(u, 1, u.s), True)

    def st5(k):
        for u in each(k):
            got(u, 4, r2[u.a].at[1, :, u.cols])
            got(u, 5, r2[u.a].at[2, :, u.cols])
            rc = RC[u.a]
            t = a1[u.a][pos[axis(u, 1)], :, u.cols] + r2[u.a][1, :, u.cols].astype(F32) + r2[u.a][2, :, u.cols].astype(F32)
            for q in range(4):
                a2[u.a][q, 0:rc, u.cols] = t[rc * q : rc * q + rc]
            sum3(u, 0, at(u, 2, 2), False)
        for u in each(k):
            sum3(u, 1, at(u, 2, -u.s), False)

    def st6(k):
        for u in each(k):
            got(u, 6, r3[u.a].at[0, :, u.cols])
            sum3(u, 2, at(u, 2, u.s), True)

    def st7(k):
        for u in each(k):
            got(u, 7, r3[u.a].at[1, :, u.cols])
            got(u, 8, r3[u.a].at[2, :, u.cols])
            h = H[u.a]
            t = a2[u.a][pos[axis(u, 2)], :, u.cols] + r3[u.a][1, :, u.cols].astype(F32) + r3[u.a][2, :, u.cols].astype(F32)
            for q in range(2):
                gs[u.a][q, 0:h, u.cols] = t[h * q : h * q + h].astype(BF)
            post(u, 9, gs[u.a].at[1 - c, :, u.cols], gr[u.a].at[:, u.cols], partner)

    def st8(k):
        for u in each(k):
            got(u, 9, gr[u.a].at[:, u.cols])
            h = H[u.a]
            for mine in (False, True):
                layer = c if mine else 1 - c
                grad = gs[u.a][c, 0:h, u.cols] if mine else gr[u.a][0:h, u.cols]
                grad = grad.astype(F32)
                gfin[u.a][layer, :, u.cols] = grad
                new, _, _ = adamw(w[u.a][layer, :, u.cols].astype(F32), m[u.a][layer, :, u.cols], v[u.a][layer, :, u.cols], grad)
                if mine:
                    wx[u.a][c, 0:h, u.cols] = new
                else:
                    ws[u.a][0:h, u.cols] = new
                    post(u, 10, ws[u.a].at[:, u.cols], wx[u.a].at[c, :, u.cols], partner)

    def spread(u, base, phase, i, ref, q):
        post(u, base + i, ref(q), ref(q), near(axis(u, phase), -u.s if i == 1 else u.s))

    def start_spread(u, base, phase, ref):
        q = pos[axis(u, phase)]
        spread(u, base, phase, 0, ref, q)
        spread(u, base, phase, 1, ref, q)

    def pass_on(u, base, phase, ref):
        q = at(u, phase, -u.s)
        got(u, base, ref(q))
        spread(u, base, phase, 2, ref, q)

    def end_spread(u, base, phase, ref):
        got(u, base + 1, ref(at(u, phase, u.s)))
        got(u, base + 2, ref(at(u, phase, 2)))

    def ref3(u):
        return lambda q: ag3[u.a].at[q, :, u.cols]

    def ref2(u):
        if u.a == 0:
            return lambda q: out[0].at[c, pos[0], q, :, u.cols]
        if u.a == 1:
            return lambda q: ag2u.at[q, :, u.cols]
        return lambda q: out[2].at[c, pos[2], q, :, u.cols]

    def ref1(u):
        if u.a == 1:
            return lambda q: out[1].at[c, :, q, :, u.cols]
        return lambda q: out[u.a].at[c, q, :, :, u.cols]

    def st9(k):
        for u in each(k):
            got(u, 10, wx[u.a].at[1 - c, :, u.cols])
            h, rp = H[u.a], RP[u.a]
            for q in range(2):
                tmp[h * q : h * q + h, 0 : u.cn] = wx[u.a][q, 0:h, u.cols].astype(F32)
            ag3[u.a][pos[axis(u, 2)], :, u.cols] = tmp[0:rp, 0 : u.cn].astype(BF)
            start_spread(u, 11, 2, ref3(u))

    def st10(k):
        for u in each(k):
            pass_on(u, 11, 2, ref3(u))

    def st11(k):
        for u in each(k):
            end_spread(u, 11, 2, ref3(u))
            rc, r = RC[u.a], R[u.a]
            for q in range(4):
                tmp[rc * q : rc * q + rc, 0 : u.cn] = ag3[u.a][q, 0:rc, u.cols].astype(F32)
            ref2(u)(pos[axis(u, 1)])[...] = tmp[0:r, 0 : u.cn].astype(BF)
            start_spread(u, 14, 1, ref2(u))

    def st12(k):
        for u in each(k):
            pass_on(u, 14, 1, ref2(u))

    def st13(k):
        for u in each(k):
            end_spread(u, 14, 1, ref2(u))
            if u.a == 1:
                for x in range(4):
                    for z in range(4):
                        tmp[12 * z : 12 * z + 12, 0 : u.cn] = ag2u[z, 12 * x : 12 * x + 12, u.cols].astype(F32)
                    out[1][c, x, pos[1], :, u.cols] = tmp[0:48, 0 : u.cn].astype(BF)
            start_spread(u, 17, 0, ref1(u))
            over(u, 21, pos[axis(u, 0)])

    def mate(u):
        if u.a == 1:
            return lambda q: out[1].at[1 - c, :, q, :, u.cols]
        return lambda q: out[u.a].at[1 - c, q, :, :, u.cols]

    def over(u, i, q):
        post(u, i, ref1(u)(q), ref1(u)(q), partner)

    def st14(k):
        for u in each(k):
            pass_on(u, 17, 0, ref1(u))
            over(u, 22, at(u, 0, -u.s))

    def st15(k):
        for u in each(k):
            got(u, 18, ref1(u)(at(u, 0, u.s)))
            over(u, 23, at(u, 0, u.s))
        for u in each(k):
            got(u, 19, ref1(u)(at(u, 0, 2)))
            over(u, 24, at(u, 0, 2))

    def st16(k):
        for u in each(k):
            other = mate(u)
            got(u, 21, other(pos[axis(u, 0)]))
            got(u, 22, other(at(u, 0, -u.s)))
            got(u, 23, other(at(u, 0, u.s)))
            got(u, 24, other(at(u, 0, 2)))

    for k in range(CHUNKS):
        for u in each(k):
            loads(u).start()
    barrier = pltpu.get_barrier_semaphore()
    peers = [partner] + [near(x, d) for x in range(3) for d in (1, -1)]
    for peer in peers:
        pl.semaphore_signal(barrier, inc=1, device_id=(rep, peer), device_id_type=MESH)
    pl.semaphore_wait(barrier, len(peers))

    stages = (st0, st1, st2, st3, st4, st5, st6, st7, st8, st9, st10, st11, st12, st13, st14, st15, st16)
    for k in range(CHUNKS):
        st0(k)
    order = sorted((WHEN[s] + LAG * k, k, s) for s in range(1, len(stages)) for k in range(CHUNKS))
    for _, k, s in order:
        stages[s](k)
    for u, i, src in pending:
        waiter(u, i, src).wait_send()


def finish_kernel(*refs):
    it = iter(refs)

    def take(n):
        return [next(it) for _ in range(n)]

    src, g, m, v = take(3), take(3), take(3), take(3)
    out, mo, vo = take(3), take(3), take(3)
    buf, tmp, sem, bsem = take(4)
    copies = [pltpu.make_async_copy(src[a], out[a], sem.at[a]) for a in range(2)]
    for one in copies:
        one.start()
    for a in range(3):
        grad = g[a][...]
        mo[a][...] = 0.9 * m[a][...] + 0.1 * grad
        vo[a][...] = 0.95 * v[a][...] + 0.05 * grad * grad

    def back(layer, x, n):
        return pltpu.make_async_copy(buf.at[n], out[2].at[layer, x], bsem.at[n])

    for layer in range(2):
        for x in range(4):
            n = 4 * layer + x

            @pl.loop(0, 3)
            def _(j):
                cols = pl.ds(pl.multiple_of(j * 256, 256), 256)
                for y in range(4):
                    for z in range(4):
                        tmp[28 * z : 28 * z + 28] = src[2][layer, z, x, 28 * y : 28 * y + 28, cols].astype(F32)
                    buf[n, y, :, cols] = tmp[...].astype(BF)

            back(layer, x, n).start()
    for layer in range(2):
        for x in range(4):
            back(layer, x, 4 * layer + x).wait()
    for one in copies:
        one.wait()


def solution(mesh):
    def step(*arrays):
        terms, weights, m, v = (arrays[i : i + 3] for i in (0, 3, 6, 9))
        me = lax.axis_index("dp")
        terms = [t[0].reshape(2, 4, 4, R[a], COLS[a]) for a, t in enumerate(terms)]
        own = [lax.dynamic_slice_in_dim(w, me * one.shape[1], one.shape[1], 1) for w, one in zip(weights, m, strict=True)]
        vmem = pl.BlockSpec(memory_space=pltpu.VMEM)
        hbm = pl.BlockSpec(memory_space=pl.ANY)
        per = lambda fn, dt: [pltpu.VMEM(fn(a), dt) for a in range(3)]
        whole = [(2, 4, 4, R[a], COLS[a]) for a in range(3)]
        n = len(units())
        scratch = (
            per(lambda a: (4, 4, R[a], COLS[a]), BF) * 2
            + [pltpu.VMEM((4, 4, R[2], COLS[2]), F32)]
            + per(lambda a: (3, 4, R[a], COLS[a]), BF) * 2
            + per(lambda a: (4, R[a], COLS[a]), F32)
            + per(lambda a: (3, R[a], COLS[a]), BF) * 2
            + per(lambda a: (4, RP[a], COLS[a]), F32)
            + per(lambda a: (3, RP[a], COLS[a]), BF) * 2
            + per(lambda a: (2, 16, COLS[a]), BF)
            + per(lambda a: (16, COLS[a]), BF)
            + per(lambda a: (2, 16, COLS[a]), BF)
            + per(lambda a: (16, COLS[a]), BF)
            + per(lambda a: (4, RP[a], COLS[a]), BF)
            + [pltpu.VMEM((4, 48, COLS[1]), BF), pltpu.VMEM((112, 128 * max(max(t) for t in TILES)), F32)]
            + [pltpu.SemaphoreType.DMA((n,)), pltpu.SemaphoreType.DMA((n, MSGS)), pltpu.SemaphoreType.DMA((n, MSGS))]
        )
        got = pl.pallas_call(
            comm_kernel,
            out_shape=[pltpu.VMEM(s, BF) for s in whole] + [jax.ShapeDtypeStruct((2, H[a], COLS[a]), F32) for a in range(3)],
            in_specs=[hbm] * 3 + [vmem] * 9,
            out_specs=[vmem] * 6,
            scratch_shapes=scratch,
            compiler_params=pltpu.CompilerParams(collective_id=0, has_side_effects=True, vmem_limit_bytes=48_500_000),
        )(*terms, *own, *m, *v)
        kept = [pltpu.with_memory_space_constraint(x, pltpu.VMEM) for x in got[:3]]
        shapes = [jax.ShapeDtypeStruct(s, BF) for s in whole] + [jax.ShapeDtypeStruct((2, H[a], COLS[a]), F32) for a in range(3)] * 2
        done = pl.pallas_call(
            finish_kernel,
            out_shape=shapes,
            in_specs=[vmem] * 12,
            out_specs=[hbm] * 3 + [vmem] * 6,
            scratch_shapes=[
                pltpu.VMEM((8, 4, R[2], COLS[2]), BF),
                pltpu.VMEM((112, 256), F32),
                pltpu.SemaphoreType.DMA((2,)),
                pltpu.SemaphoreType.DMA((8,)),
            ],
            compiler_params=pltpu.CompilerParams(vmem_limit_bytes=20_000_000),
        )(*kept, *got[3:], *m, *v)
        return [x.reshape(w.shape) for x, w in zip(done[:3], weights, strict=True)] + list(done[3:])

    def run(*arrays):
        return tuple(step(*arrays))

    all_of, cut = P(None, None, None), P(None, "dp", None)
    return jax.shard_map(
        run,
        mesh=mesh,
        in_specs=(P(("rep", "dp"), None, None, None),) * 3 + (all_of,) * 3 + (cut,) * 6,
        out_specs=(P("rep", None, None),) * 3 + (P("rep", "dp", None),) * 6,
        check_vma=False,
    )
```

```python
import jax
import jax.numpy as jnp
from jax import lax
from jax.experimental import pallas as pl
from jax.experimental.pallas import tpu as pltpu
from jax.sharding import PartitionSpec as P

MESH = pl.DeviceIdType.MESH
BF, F32 = jnp.bfloat16, jnp.float32

COLS = (1792, 1792, 768)
R = (48, 48, 112)
RC = (12, 12, 28)
RP = (16, 16, 32)
H = (6, 6, 14)
AXES = ((0, 1, 2), (1, 2, 0), (2, 0, 1))
TILES = ((2, 2, 3), (2, 2, 3), (1, 1, 1))
MSGS = 25
VMEM_LIMIT = 49_500_000
ORDER = (
    1, 193, 33, 385, 225, 417, 2, 97, 257, 194, 34, 65, 481, 226, 3, 129, 418, 321, 386, 35, 195, 545, 4, 66,
    98, 258, 353, 482, 419, 227, 161, 322, 36, 130, 196, 5, 449, 546, 289, 67, 99, 354, 420, 259, 513, 483, 260, 450,
    421, 387, 100, 37, 484, 197, 162, 6, 290, 131, 323, 388, 355, 261, 514, 547, 198, 485, 451, 422, 101, 68, 228, 38,
    7, 132, 291, 389, 262, 356, 486, 8, 324, 163, 423, 452, 229, 102, 9, 548, 69, 199, 390, 263, 292, 39, 133, 357,
    515, 424, 264, 230, 164, 325, 70, 103, 200, 487, 425, 40, 10, 391, 358, 453, 549, 293, 134, 516, 41, 488, 201, 231,
    104, 265, 426, 165, 326, 71, 359, 489, 294, 550, 232, 105, 42, 72, 360, 202, 517, 427, 392, 166, 327, 135, 11, 361,
    454, 73, 551, 393, 490, 233, 295, 328, 43, 203, 518, 106, 552, 167, 136, 296, 362, 428, 455, 329, 74, 394, 168, 553,
    297, 137, 12, 44, 204, 491, 169, 107, 363, 266, 456, 330, 519, 429, 395, 234, 298, 554, 75, 457, 45, 205, 138, 108,
    520, 170, 364, 396, 331, 492, 76, 235, 13, 521, 458, 267, 299, 171, 139, 555, 430, 46, 47, 332, 109, 522, 365, 397,
    14, 15, 523, 556, 268, 459, 172, 493, 333, 431, 432, 300, 236, 398, 269, 77, 110, 140, 206, 366, 367, 524, 557, 460,
    334, 173, 494, 16, 525, 301, 461, 141, 111, 112, 433, 207, 399, 78, 270, 17, 237, 48, 558, 79, 526, 400, 174, 175,
    208, 302, 113, 142, 462, 401, 238, 368, 495, 496, 80, 559, 335, 527, 209, 369, 336, 528, 49, 143, 303, 304, 271, 272,
    463, 176, 560, 464, 529, 144, 239, 240, 337, 497, 81, 561, 273, 177, 465, 145, 305, 241,
)


def adamw(w, m, v, g):
    m = 0.9 * m + 0.1 * g
    v = 0.95 * v + 0.05 * g * g
    step = m * lax.rsqrt(v + 1e-8) + 0.1 * w
    return (w - 0.02 * step).astype(BF), m, v


class Unit:
    def __init__(self, color, chunk, way, c0, cn, uid):
        self.a, self.chunk, self.s, self.c0, self.cn, self.u = color, chunk, way, c0, cn, uid
        self.cols = pl.ds(c0, cn)


def units():
    found, uid = [], 0
    for a in range(3):
        c0 = 0
        for k, t in enumerate(TILES[a]):
            for way in (1, -1):
                found.append(Unit(a, k, way, c0, 128 * t, uid))
                c0 += 128 * t
                uid += 1
        assert c0 == COLS[a]
    return found


def comm_kernel(*refs):
    it = iter(refs)

    def take(n):
        return [next(it) for _ in range(n)]

    g, wh, mh, vh = take(3), take(3), take(3), take(3)
    out, mo, vo = take(3), take(3), take(3)
    own, part = take(3), take(3)
    psum = next(it)
    s1, r1, a1, s2, r2, a2, s3, r3 = (take(3) for _ in range(8))
    gs, gg, wx, wn, ag3, wz, wsel, m, v = (take(3) for _ in range(9))
    ag2u, tmp, osem, msem, ssem, rsem = take(6)
    all_units = units()

    me = lax.axis_index("dp")
    rep = lax.axis_index("rep")
    c = lax.rem(me, 2)
    pos = (me // 32, lax.rem(me // 8, 4), lax.rem(me // 2, 4))
    strides = (32, 8, 2)
    partner = me + 1 - 2 * c

    def near(axis, d):
        return me + (lax.rem(pos[axis] + d + 4, 4) - pos[axis]) * strides[axis]

    def send(u, i, src, dst, to):
        pltpu.make_async_remote_copy(
            src_ref=src, dst_ref=dst, send_sem=ssem.at[u.u, i], recv_sem=rsem.at[u.u, i], device_id=(rep, to), device_id_type=MESH
        ).start()

    def waiter(u, i, ref):
        return pltpu.make_async_remote_copy(
            src_ref=ref, dst_ref=ref, send_sem=ssem.at[u.u, i], recv_sem=rsem.at[u.u, i], device_id=(rep, partner), device_id_type=MESH
        )

    pending = []

    def post(u, i, src, dst, to):
        send(u, i, src, dst, to)
        pending.append((u, i, src))

    def got(u, i, ref):
        waiter(u, i, ref).wait_recv()

    def loads(u):
        return pltpu.make_async_copy(g[u.a].at[c, :, :, :, u.cols], own[u.a].at[:, :, :, u.cols], osem.at[u.u])

    def mine1(u, q, i):
        if u.a == 2:
            return psum[q, i, :, u.cols]
        at = (q, i) if u.a == 0 else (i, q)
        return own[u.a][(*at, slice(None), u.cols)].astype(F32) + part[u.a][(*at, slice(None), u.cols)].astype(F32)

    def axis(u, phase):
        return AXES[u.a][phase]

    def at(u, phase, d):
        return lax.rem(pos[axis(u, phase)] + d + 4, 4)

    S = slice(None)

    def sum1(u, i, q, came):
        @pl.loop(0, 4)
        def _(j):
            x = mine1(u, q, j)
            if came:
                x = x + r1[u.a][0, j, :, u.cols].astype(F32)
            s1[u.a][i, j, :, u.cols] = x.astype(BF)

        post(u, i, s1[u.a].at[i, :, :, u.cols], r1[u.a].at[i, :, :, u.cols], near(axis(u, 0), -u.s if i == 1 else u.s))

    def sum2(u, i, q, came):
        x = a1[u.a][q, :, u.cols]
        if came:
            x = x + r2[u.a][0, :, u.cols].astype(F32)
        s2[u.a][i, :, u.cols] = x.astype(BF)
        post(u, 3 + i, s2[u.a].at[i, :, u.cols], r2[u.a].at[i, :, u.cols], near(axis(u, 1), -u.s if i == 1 else u.s))

    def sum3(u, i, q, came):
        x = a2[u.a][q, :, u.cols]
        if came:
            x = x + r3[u.a][0, :, u.cols].astype(F32)
        s3[u.a][i, :, u.cols] = x.astype(BF)
        post(u, 6 + i, s3[u.a].at[i, :, u.cols], r3[u.a].at[i, :, u.cols], near(axis(u, 2), -u.s if i == 1 else u.s))

    def start_sum(u, phase, fn):
        fn(u, 0, at(u, phase, 2), False)
        fn(u, 1, at(u, phase, -u.s), False)

    def st0(u):
        post(u, 20, g[u.a].at[1 - c, :, :, :, u.cols], part[u.a].at[:, :, :, u.cols], partner)

    def st1(u):
        loads(u).wait()
        got(u, 20, part[u.a].at[:, :, :, u.cols])
        if u.a == 2:

            @pl.loop(0, 4)
            def _(x):
                for y in range(4):
                    t = own[2][x, y, :, u.cols].astype(F32) + part[2][x, y, :, u.cols].astype(F32)
                    for z in range(4):
                        psum[z, x, 28 * y : 28 * y + 28, u.cols] = t[28 * z : 28 * z + 28]

        start_sum(u, 0, sum1)

    def st2(u):
        got(u, 0, r1[u.a].at[0, :, :, u.cols])
        sum1(u, 2, at(u, 0, u.s), True)

    def st3(u):
        got(u, 1, r1[u.a].at[1, :, :, u.cols])
        got(u, 2, r1[u.a].at[2, :, :, u.cols])
        q = pos[axis(u, 0)]

        def total(j):
            return mine1(u, q, j) + r1[u.a][1, j, :, u.cols].astype(F32) + r1[u.a][2, j, :, u.cols].astype(F32)

        if u.a == 1:
            for j in range(4):
                t = total(j)
                for z in range(4):
                    a1[1][z, 12 * j : 12 * j + 12, u.cols] = t[12 * z : 12 * z + 12]
        else:

            @pl.loop(0, 4)
            def _(j):
                a1[u.a][j, :, u.cols] = total(j)

        start_sum(u, 1, sum2)

    def st4(u):
        got(u, 3, r2[u.a].at[0, :, u.cols])
        sum2(u, 2, at(u, 1, u.s), True)

    def st5(u):
        got(u, 4, r2[u.a].at[1, :, u.cols])
        got(u, 5, r2[u.a].at[2, :, u.cols])
        rc = RC[u.a]
        t = a1[u.a][pos[axis(u, 1)], :, u.cols] + r2[u.a][1, :, u.cols].astype(F32) + r2[u.a][2, :, u.cols].astype(F32)
        for q in range(4):
            a2[u.a][q, 0:rc, u.cols] = t[rc * q : rc * q + rc]
        start_sum(u, 2, sum3)

    def st6(u):
        got(u, 6, r3[u.a].at[0, :, u.cols])
        sum3(u, 2, at(u, 2, u.s), True)

    def st7(u):
        got(u, 7, r3[u.a].at[1, :, u.cols])
        got(u, 8, r3[u.a].at[2, :, u.cols])
        h = H[u.a]
        t = a2[u.a][pos[axis(u, 2)], :, u.cols] + r3[u.a][1, :, u.cols].astype(F32) + r3[u.a][2, :, u.cols].astype(F32)
        for q in range(2):
            gs[u.a][q, 0:h, u.cols] = t[h * q : h * q + h].astype(BF)
        post(u, 9, gs[u.a].at[1 - c, :, u.cols], gg[u.a].at[c, :, u.cols], partner)
        gg[u.a][c, 0:h, u.cols] = gs[u.a][c, 0:h, u.cols]

    def st8(u):
        got(u, 9, gg[u.a].at[1 - c, :, u.cols])
        h = H[u.a]
        for layer in range(2):
            grad = gg[u.a][layer, 0:h, u.cols].astype(F32)
            new, mn, vn = adamw(wsel[u.a][layer, 0:h, u.cols], m[u.a][:, layer, u.cols], v[u.a][:, layer, u.cols], grad)
            wn[u.a][layer, 0:h, u.cols] = new
            mo[u.a][:, layer, u.cols] = mn
            vo[u.a][:, layer, u.cols] = vn
        post(u, 10, wn[u.a].at[1 - c, :, u.cols], wx[u.a].at[c, :, u.cols], partner)

    def spread(u, base, phase, i, ref, q):
        post(u, base + i, ref(q), ref(q), near(axis(u, phase), -u.s if i == 1 else u.s))

    def start_spread(u, base, phase, ref):
        q = pos[axis(u, phase)]
        spread(u, base, phase, 0, ref, q)
        spread(u, base, phase, 1, ref, q)

    def pass_on(u, base, phase, ref):
        q = at(u, phase, -u.s)
        got(u, base, ref(q))
        spread(u, base, phase, 2, ref, q)

    def end_spread(u, base, phase, ref):
        got(u, base + 1, ref(at(u, phase, u.s)))
        got(u, base + 2, ref(at(u, phase, 2)))

    def ref3(u):
        return lambda q: ag3[u.a].at[q, :, u.cols]

    def ref2(u):
        if u.a == 0:
            return lambda q: out[0].at[c, pos[0], q, :, u.cols]
        if u.a == 1:
            return lambda q: ag2u.at[q, :, u.cols]
        return lambda q: out[2].at[c, pos[2], q, :, u.cols]

    def ref1(u, layer=c):
        if u.a == 1:
            return lambda q: out[1].at[layer, :, q, :, u.cols]
        return lambda q: out[u.a].at[layer, q, :, :, u.cols]

    def over(u, i, q):
        post(u, i, ref1(u)(q), ref1(u)(q), partner)

    def st9(u):
        got(u, 10, wx[u.a].at[1 - c, :, u.cols])
        h, rp = H[u.a], RP[u.a]
        wx[u.a][c, 0:h, u.cols] = wn[u.a][c, 0:h, u.cols]
        for q in range(2):
            tmp[h * q : h * q + h, 0 : u.cn] = wx[u.a][q, 0:h, u.cols].astype(F32)
        ag3[u.a][pos[axis(u, 2)], :, u.cols] = tmp[0:rp, 0 : u.cn].astype(BF)
        start_spread(u, 11, 2, ref3(u))

    def st10(u):
        pass_on(u, 11, 2, ref3(u))

    def st11(u):
        end_spread(u, 11, 2, ref3(u))
        rc, r = RC[u.a], R[u.a]
        for q in range(4):
            tmp[rc * q : rc * q + rc, 0 : u.cn] = ag3[u.a][q, 0:rc, u.cols].astype(F32)
        ref2(u)(pos[axis(u, 1)])[...] = tmp[0:r, 0 : u.cn].astype(BF)
        start_spread(u, 14, 1, ref2(u))

    def st12(u):
        pass_on(u, 14, 1, ref2(u))

    def st13(u):
        end_spread(u, 14, 1, ref2(u))
        if u.a == 1:
            for x in range(4):
                for z in range(4):
                    tmp[12 * z : 12 * z + 12, 0 : u.cn] = ag2u[z, 12 * x : 12 * x + 12, u.cols].astype(F32)
                out[1][c, x, pos[1], :, u.cols] = tmp[0:48, 0 : u.cn].astype(BF)
        start_spread(u, 17, 0, ref1(u))
        over(u, 21, pos[axis(u, 0)])

    def st14(u):
        pass_on(u, 17, 0, ref1(u))
        over(u, 22, at(u, 0, -u.s))

    def st15(u):
        got(u, 18, ref1(u)(at(u, 0, u.s)))
        over(u, 23, at(u, 0, u.s))

    def st16(u):
        got(u, 19, ref1(u)(at(u, 0, 2)))
        over(u, 24, at(u, 0, 2))

    def st17(u):
        theirs = ref1(u, 1 - c)
        got(u, 21, theirs(pos[axis(u, 0)]))
        got(u, 22, theirs(at(u, 0, -u.s)))
        got(u, 23, theirs(at(u, 0, u.s)))
        got(u, 24, theirs(at(u, 0, 2)))

    small = []
    for a in range(3):
        for src, dst in (
            (wh[a].at[:, pos[0], pos[1]], wz[a]),
            (mh[a], m[a]),
            (vh[a], v[a]),
        ):
            small.append(pltpu.make_async_copy(src, dst, msem.at[len(small)]))
    by_chunk = sorted(all_units, key=lambda u: (u.chunk, u.u))
    for u in by_chunk:
        loads(u).start()
    barrier = pltpu.get_barrier_semaphore()
    peers = [partner] + [near(x, d) for x in range(3) for d in (1, -1)]
    for peer in peers:
        pl.semaphore_signal(barrier, inc=1, device_id=(rep, peer), device_id_type=MESH)
    pl.semaphore_wait(barrier, len(peers))

    for u in by_chunk:
        st0(u)
    for one in small:
        one.start()
    for one in small:
        one.wait()
    rank = lax.rem(me, 8)
    for a in range(3):

        @pl.loop(0, COLS[a] // 256)
        def _(j):
            cols = pl.ds(pl.multiple_of(j * 256, 256), 256)
            h = H[a]
            for layer in range(2):
                line = wz[a][layer, :, cols].astype(F32)
                mine = line[0:h]
                for q in range(1, 8):
                    mine = jnp.where(rank == q, line[h * q : h * q + h], mine)
                wsel[a][layer, 0:h, cols] = mine

    stages = (st0, st1, st2, st3, st4, st5, st6, st7, st8, st9, st10, st11, st12, st13, st14, st15, st16, st17)
    for code in ORDER:
        stages[code % 32](all_units[code // 32])
    for u, i, src in pending:
        waiter(u, i, src).wait_send()


def finish_kernel(*refs):
    it = iter(refs)

    def take(n):
        return [next(it) for _ in range(n)]

    src, moments, out, new = take(3), take(6), take(3), take(6)
    buf, tmp, sem, bsem = take(4)
    copies = [pltpu.make_async_copy(x, y, sem.at[i]) for i, (x, y) in enumerate(zip(src[:2] + moments, out[:2] + new, strict=True))]
    for one in copies:
        one.start()

    def back(layer, x, n):
        return pltpu.make_async_copy(buf.at[n], out[2].at[layer, x], bsem.at[n])

    for layer in range(2):
        for x in range(4):
            n = 4 * layer + x

            @pl.loop(0, 3)
            def _(j):
                cols = pl.ds(pl.multiple_of(j * 256, 256), 256)
                for y in range(4):
                    for z in range(4):
                        tmp[28 * z : 28 * z + 28] = src[2][layer, z, x, 28 * y : 28 * y + 28, cols].astype(F32)
                    buf[n, y, :, cols] = tmp[...].astype(BF)

            back(layer, x, n).start()
    for layer in range(2):
        for x in range(4):
            back(layer, x, 4 * layer + x).wait()
    for one in copies:
        one.wait()


def solution(mesh):
    def step(*arrays):
        terms, weights, m, v = (arrays[i : i + 3] for i in (0, 3, 6, 9))
        whole = [(2, 4, 4, R[a], COLS[a]) for a in range(3)]
        terms = [t[0].reshape(s) for t, s in zip(terms, whole, strict=True)]
        views = [w.reshape(s) for w, s in zip(weights, whole, strict=True)]
        m, v = ([x.transpose(1, 0, 2) for x in y] for y in (m, v))
        vmem = pl.BlockSpec(memory_space=pltpu.VMEM)
        hbm = pl.BlockSpec(memory_space=pl.ANY)
        per = lambda fn, dt: [pltpu.VMEM(fn(a), dt) for a in range(3)]
        moment = lambda a: (H[a], 2, COLS[a])
        rows = lambda a: (2, 16, COLS[a])
        n = len(units())
        scratch = (
            per(lambda a: (4, 4, R[a], COLS[a]), BF) * 2
            + [pltpu.VMEM((4, 4, R[2], COLS[2]), F32)]
            + per(lambda a: (3, 4, R[a], COLS[a]), BF) * 2
            + per(lambda a: (4, R[a], COLS[a]), F32)
            + per(lambda a: (3, R[a], COLS[a]), BF) * 2
            + per(lambda a: (4, RP[a], COLS[a]), F32)
            + per(lambda a: (3, RP[a], COLS[a]), BF) * 2
            + per(rows, BF) * 4
            + per(lambda a: (4, RP[a], COLS[a]), BF)
            + per(lambda a: (2, R[a], COLS[a]), BF)
            + per(lambda a: (2, 8 if a < 2 else 16, COLS[a]), F32)
            + per(moment, F32) * 2
            + [pltpu.VMEM((4, 48, COLS[1]), BF), pltpu.VMEM((112, 128 * max(max(t) for t in TILES)), F32)]
            + [pltpu.SemaphoreType.DMA((n,)), pltpu.SemaphoreType.DMA((9,)), pltpu.SemaphoreType.DMA((n, MSGS)), pltpu.SemaphoreType.DMA((n, MSGS))]
        )
        got = pl.pallas_call(
            comm_kernel,
            out_shape=[pltpu.VMEM(s, BF) for s in whole] + per(moment, F32) * 2,
            in_specs=[hbm] * 12,
            out_specs=[vmem] * 9,
            scratch_shapes=scratch,
            compiler_params=pltpu.CompilerParams(collective_id=0, has_side_effects=True, vmem_limit_bytes=VMEM_LIMIT),
        )(*terms, *views, *m, *v)
        kept = [pltpu.with_memory_space_constraint(x, pltpu.VMEM) for x in got]
        done = pl.pallas_call(
            finish_kernel,
            out_shape=[jax.ShapeDtypeStruct(s, BF) for s in whole] + [jax.ShapeDtypeStruct(moment(a), F32) for a in range(3)] * 2,
            in_specs=[vmem] * 9,
            out_specs=[hbm] * 9,
            scratch_shapes=[
                pltpu.VMEM((8, 4, R[2], COLS[2]), BF),
                pltpu.VMEM((112, 256), F32),
                pltpu.SemaphoreType.DMA((8,)),
                pltpu.SemaphoreType.DMA((8,)),
            ],
            compiler_params=pltpu.CompilerParams(vmem_limit_bytes=20_000_000),
        )(*kept)
        return [x.reshape(w.shape) for x, w in zip(done[:3], weights, strict=True)] + [x.transpose(1, 0, 2) for x in done[3:]]

    def run(*arrays):
        return tuple(step(*arrays))

    all_of, cut = P(None, None, None), P(None, "dp", None)
    return jax.shard_map(
        run,
        mesh=mesh,
        in_specs=(P(("rep", "dp"), None, None, None),) * 3 + (all_of,) * 3 + (cut,) * 6,
        out_specs=(P("rep", None, None),) * 3 + (P("rep", "dp", None),) * 6,
        check_vma=False,
    )
```

```python
import jax
import jax.numpy as jnp
from jax import lax
from jax.experimental import pallas as pl
from jax.experimental.pallas import tpu as pltpu
from jax.sharding import PartitionSpec as P

MESH = pl.DeviceIdType.MESH
BF, F32 = jnp.bfloat16, jnp.float32

COLS = (1792, 1792, 768)
R = (48, 48, 112)
RC = (12, 12, 28)
RP = (16, 16, 32)
H = (6, 6, 14)
AXES = ((0, 1, 2), (1, 2, 0), (2, 0, 1))
TILES = ((2, 2, 3), (2, 2, 3), (1, 1, 1))
VMEM_LIMIT = 49_500_000
ORDER = (
    1, 97, 193, 33, 129, 98, 225, 2, 194, 34, 130, 161, 65, 226, 99, 131, 35, 195, 3, 257, 162, 66, 132, 196,
    100, 227, 258, 36, 4, 197, 67, 228, 133, 163, 37, 198, 5, 101, 259, 229, 134, 68, 164, 199, 38, 6, 102, 260,
    230, 200, 135, 69, 165, 39, 201, 7, 103, 136, 231, 261, 40, 166, 70, 137, 41, 262, 104, 202, 232, 8, 138, 167,
    71, 105, 42, 9, 233, 263, 168, 203, 72, 139, 264, 43, 169, 10, 106, 234, 73, 140, 265, 204, 170, 44, 107, 11,
    235, 266, 141, 74, 171, 45, 108, 205, 75, 267, 236, 12, 142, 46, 172, 76, 109, 206, 268, 13, 237, 173, 77, 269,
    238, 110, 47, 14, 15, 78, 174, 143, 144, 270, 111, 175, 271, 48, 207, 208, 112, 16, 79, 239, 240, 176, 272, 17,
    80, 145, 209, 241, 49, 113, 177, 273, 81,
)


def adamw(w, m, v, g):
    m = 0.9 * m + 0.1 * g
    v = 0.95 * v + 0.05 * g * g
    step = m * lax.rsqrt(v + 1e-8) + 0.1 * w
    return (w - 0.02 * step).astype(BF), m, v


class Unit:
    def __init__(self, way, c0, cn):
        self.s, self.cn, self.cols = way, cn, pl.ds(c0, cn)


class Pair:
    def __init__(self, color, chunk, uid, c0, cn):
        self.a, self.chunk, self.p, self.cn, self.cols = color, chunk, uid, cn, pl.ds(c0, cn)
        self.units = (Unit(1, c0, cn // 2), Unit(-1, c0 + cn // 2, cn // 2))


def pairs():
    found = []
    for a in range(3):
        c0 = 0
        for k, t in enumerate(TILES[a]):
            found.append(Pair(a, k, len(found), c0, 256 * t))
            c0 += 256 * t
    return found


RECV = (0, 1, 2, 3, 4, 5, 6, 7, 8, 10, 9, 3, 4, 5, 0, 1, 2, 11, 12, 13, 9, 10, 14, 15, 16)
SEND = (0, 1, 2, 0, 1, 2, 0, 1, 2, 3, 3, 0, 1, 2, 0, 1, 2, 0, 1, 2, 3, 3, 4, 5, 6)


def comm_kernel(*refs):
    it = iter(refs)

    def take(n):
        return [next(it) for _ in range(n)]

    g, wh, mh, vh = take(3), take(3), take(3), take(3)
    out, mo, vo = take(3), take(3), take(3)
    own, part = take(3), take(3)
    psum = next(it)
    s1, r1, a1, s2, r2, a2, s3, r3 = (take(3) for _ in range(8))
    gs, gg, wx, wn, ag3, wz, wsel, m, v = (take(3) for _ in range(9))
    ag2u, tmp, osem, msem, ssem, rsem = take(6)
    all_pairs = pairs()

    me = lax.axis_index("dp")
    rep = lax.axis_index("rep")
    c = lax.rem(me, 2)
    pos = (me // 32, lax.rem(me // 8, 4), lax.rem(me // 2, 4))
    strides = (32, 8, 2)
    partner = me + 1 - 2 * c

    def near(axis, d):
        return me + (lax.rem(pos[axis] + d + 4, 4) - pos[axis]) * strides[axis]

    def message(u, i, src, dst, to):
        return pltpu.make_async_remote_copy(
            src_ref=src, dst_ref=dst, send_sem=ssem.at[u.p, SEND[i]], recv_sem=rsem.at[u.p, RECV[i]], device_id=(rep, to), device_id_type=MESH
        )

    leaving = {}

    def post(u, i, sends, whole):
        key = (u.p, SEND[i])
        if key in leaving:
            leaving.pop(key)()
        for one in sends:
            message(u, i, *one).start()
        leaving[key] = lambda: message(u, i, whole, whole, partner).wait_send()

    def got(u, i, whole):
        message(u, i, whole, whole, partner).wait_recv()

    def loads(u):
        return pltpu.make_async_copy(g[u.a].at[c, :, :, :, u.cols], own[u.a].at[:, :, :, u.cols], osem.at[u.p])

    def mine1(u, cols, q, i):
        if u.a == 2:
            return psum[q, i, :, cols]
        where = (q, i) if u.a == 0 else (i, q)
        return own[u.a][(*where, slice(None), cols)].astype(F32) + part[u.a][(*where, slice(None), cols)].astype(F32)

    def mine2(u, cols, q, i):
        return a1[u.a][q, :, cols]

    def mine3(u, cols, q, i):
        return a2[u.a][q, :, cols]

    def axis(u, phase):
        return AXES[u.a][phase]

    def at(u, phase, d):
        return lax.rem(pos[axis(u, phase)] + d + 4, 4)

    mines, outs, ins = (mine1, mine2, mine3), (s1, s2, s3), (r1, r2, r3)

    def add(u, cols, phase, i, q):
        src, dst = ins[phase][u.a], outs[phase][u.a]
        if phase == 0:

            @pl.loop(0, 4)
            def _(j):
                x = mine1(u, cols, q, j)
                if i == 2:
                    x = x + src[0, j, :, cols].astype(F32)
                dst[i, j, :, cols] = x.astype(BF)

        else:
            x = mines[phase](u, cols, q, 0)
            if i == 2:
                x = x + src[0, :, cols].astype(F32)
            dst[i, :, cols] = x.astype(BF)

    def view(ref, phase, i, cols):
        return ref.at[i, :, :, cols] if phase == 0 else ref.at[i, :, cols]

    def give(u, phase, i):
        src, dst = outs[phase][u.a], ins[phase][u.a]
        if i == 0:
            add(u, u.cols, phase, 0, at(u, phase, 2))
        else:
            for t in u.units:
                add(u, t.cols, phase, i, at(u, phase, -t.s if i == 1 else t.s))
        sends = [(view(src, phase, i, t.cols), view(dst, phase, i, t.cols), near(axis(u, phase), -t.s if i == 1 else t.s)) for t in u.units]
        post(u, 3 * phase + i, sends, view(src, phase, i, u.cols))

    def take_in(u, phase, i):
        got(u, 3 * phase + i, view(ins[phase][u.a], phase, i, u.cols))

    def st0(u):
        post(u, 20, [(g[u.a].at[1 - c, :, :, :, u.cols], part[u.a].at[:, :, :, u.cols], partner)], part[u.a].at[:, :, :, u.cols])

    def st1(u):
        loads(u).wait()
        got(u, 20, part[u.a].at[:, :, :, u.cols])
        if u.a == 2:

            @pl.loop(0, 4)
            def _(x):
                for y in range(4):
                    t = own[2][x, y, :, u.cols].astype(F32) + part[2][x, y, :, u.cols].astype(F32)
                    for z in range(4):
                        psum[z, x, 28 * y : 28 * y + 28, u.cols] = t[28 * z : 28 * z + 28]

        give(u, 0, 0)
        give(u, 0, 1)

    def st2(u):
        take_in(u, 0, 0)
        give(u, 0, 2)

    def st3(u):
        take_in(u, 0, 1)
        take_in(u, 0, 2)
        q = pos[axis(u, 0)]

        def total(j):
            return mine1(u, u.cols, q, j) + r1[u.a][1, j, :, u.cols].astype(F32) + r1[u.a][2, j, :, u.cols].astype(F32)

        if u.a == 1:
            for j in range(4):
                t = total(j)
                for z in range(4):
                    a1[1][z, 12 * j : 12 * j + 12, u.cols] = t[12 * z : 12 * z + 12]
        else:

            @pl.loop(0, 4)
            def _(j):
                a1[u.a][j, :, u.cols] = total(j)

        give(u, 1, 0)
        give(u, 1, 1)

    def st4(u):
        take_in(u, 1, 0)
        give(u, 1, 2)

    def st5(u):
        take_in(u, 1, 1)
        take_in(u, 1, 2)
        rc = RC[u.a]
        t = a1[u.a][pos[axis(u, 1)], :, u.cols] + r2[u.a][1, :, u.cols].astype(F32) + r2[u.a][2, :, u.cols].astype(F32)
        for q in range(4):
            a2[u.a][q, 0:rc, u.cols] = t[rc * q : rc * q + rc]
        give(u, 2, 0)
        give(u, 2, 1)

    def st6(u):
        take_in(u, 2, 0)
        give(u, 2, 2)

    def st7(u):
        take_in(u, 2, 1)
        take_in(u, 2, 2)
        h = H[u.a]
        t = a2[u.a][pos[axis(u, 2)], :, u.cols] + r3[u.a][1, :, u.cols].astype(F32) + r3[u.a][2, :, u.cols].astype(F32)
        for q in range(2):
            gs[u.a][q, 0:h, u.cols] = t[h * q : h * q + h].astype(BF)
        post(u, 9, [(gs[u.a].at[1 - c, :, u.cols], gg[u.a].at[c, :, u.cols], partner)], gs[u.a].at[0, :, u.cols])
        gg[u.a][c, 0:h, u.cols] = gs[u.a][c, 0:h, u.cols]

    def st8(u):
        got(u, 9, gg[u.a].at[1 - c, :, u.cols])
        h = H[u.a]
        for layer in range(2):
            grad = gg[u.a][layer, 0:h, u.cols].astype(F32)
            new, mn, vn = adamw(wsel[u.a][layer, 0:h, u.cols], m[u.a][:, layer, u.cols], v[u.a][:, layer, u.cols], grad)
            wn[u.a][layer, 0:h, u.cols] = new
            mo[u.a][:, layer, u.cols] = mn
            vo[u.a][:, layer, u.cols] = vn
        post(u, 10, [(wn[u.a].at[1 - c, :, u.cols], wx[u.a].at[c, :, u.cols], partner)], wn[u.a].at[0, :, u.cols])

    def ref3(u, cols):
        return lambda q: ag3[u.a].at[q, :, cols]

    def ref2(u, cols):
        if u.a == 0:
            return lambda q: out[0].at[c, pos[0], q, :, cols]
        if u.a == 1:
            return lambda q: ag2u.at[q, :, cols]
        return lambda q: out[2].at[c, pos[2], q, :, cols]

    def ref1(u, cols, layer=c):
        if u.a == 1:
            return lambda q: out[1].at[layer, :, q, :, cols]
        return lambda q: out[u.a].at[layer, q, :, :, cols]

    refs_of = (ref1, ref2, ref3)

    def base(phase):
        return 17 - 3 * phase

    def spread(u, phase, i):
        sends = []
        for t in u.units:
            block = refs_of[phase](u, t.cols)(at(u, phase, -t.s) if i == 2 else pos[axis(u, phase)])
            sends.append((block, block, near(axis(u, phase), -t.s if i == 1 else t.s)))
        post(u, base(phase) + i, sends, refs_of[phase](u, u.cols)(pos[axis(u, phase)]))

    def start_spread(u, phase):
        spread(u, phase, 0)
        spread(u, phase, 1)

    def arrived(u, phase, i):
        got(u, base(phase) + i, refs_of[phase](u, u.cols)(at(u, phase, 2)))

    def pass_on(u, phase):
        arrived(u, phase, 0)
        spread(u, phase, 2)

    def end_spread(u, phase):
        arrived(u, phase, 1)
        arrived(u, phase, 2)

    def over(u, i, d):
        if d % 2 == 0:
            block = ref1(u, u.cols)(at(u, 0, d))
            sends = [(block, block, partner)]
        else:
            own_blocks = [ref1(u, t.cols)(at(u, 0, d * t.s)) for t in u.units]
            sends = [(x, x, partner) for x in own_blocks]
        post(u, i, sends, ref1(u, u.cols)(pos[axis(u, 0)]))

    def st9(u):
        got(u, 10, wx[u.a].at[1 - c, :, u.cols])
        h, rp = H[u.a], RP[u.a]
        wx[u.a][c, 0:h, u.cols] = wn[u.a][c, 0:h, u.cols]
        for q in range(2):
            tmp[h * q : h * q + h, 0 : u.cn] = wx[u.a][q, 0:h, u.cols].astype(F32)
        ag3[u.a][pos[axis(u, 2)], :, u.cols] = tmp[0:rp, 0 : u.cn].astype(BF)
        start_spread(u, 2)

    def st10(u):
        pass_on(u, 2)

    def st11(u):
        end_spread(u, 2)
        rc, r = RC[u.a], R[u.a]
        for q in range(4):
            tmp[rc * q : rc * q + rc, 0 : u.cn] = ag3[u.a][q, 0:rc, u.cols].astype(F32)
        ref2(u, u.cols)(pos[axis(u, 1)])[...] = tmp[0:r, 0 : u.cn].astype(BF)
        start_spread(u, 1)

    def st12(u):
        pass_on(u, 1)

    def st13(u):
        end_spread(u, 1)
        if u.a == 1:
            for x in range(4):
                for z in range(4):
                    tmp[12 * z : 12 * z + 12, 0 : u.cn] = ag2u[z, 12 * x : 12 * x + 12, u.cols].astype(F32)
                out[1][c, x, pos[1], :, u.cols] = tmp[0:48, 0 : u.cn].astype(BF)
        start_spread(u, 0)
        over(u, 21, 0)

    def st14(u):
        pass_on(u, 0)
        over(u, 22, -1)

    def st15(u):
        arrived(u, 0, 1)
        over(u, 23, 1)

    def st16(u):
        arrived(u, 0, 2)
        over(u, 24, 2)

    def st17(u):
        for i in (21, 22, 23, 24):
            got(u, i, ref1(u, u.cols, 1 - c)(pos[axis(u, 0)]))

    small = []
    for a in range(3):
        for src, dst in (
            (wh[a].at[:, pos[0], pos[1]], wz[a]),
            (mh[a], m[a]),
            (vh[a], v[a]),
        ):
            small.append(pltpu.make_async_copy(src, dst, msem.at[len(small)]))
    by_chunk = sorted(all_pairs, key=lambda u: (u.chunk, u.p))
    for u in by_chunk:
        loads(u).start()
    barrier = pltpu.get_barrier_semaphore()
    peers = [partner] + [near(x, d) for x in range(3) for d in (1, -1)]
    for peer in peers:
        pl.semaphore_signal(barrier, inc=1, device_id=(rep, peer), device_id_type=MESH)
    pl.semaphore_wait(barrier, len(peers))

    for u in by_chunk:
        st0(u)
    for one in small:
        one.start()
    for one in small:
        one.wait()
    rank = lax.rem(me, 8)
    for a in range(3):

        @pl.loop(0, COLS[a] // 256)
        def _(j):
            cols = pl.ds(pl.multiple_of(j * 256, 256), 256)
            h = H[a]
            for layer in range(2):
                line = wz[a][layer, :, cols].astype(F32)
                mine = line[0:h]
                for q in range(1, 8):
                    mine = jnp.where(rank == q, line[h * q : h * q + h], mine)
                wsel[a][layer, 0:h, cols] = mine

    stages = (st0, st1, st2, st3, st4, st5, st6, st7, st8, st9, st10, st11, st12, st13, st14, st15, st16, st17)
    for code in ORDER:
        stages[code % 32](all_pairs[code // 32])
    for wait in leaving.values():
        wait()


def finish_kernel(*refs):
    it = iter(refs)

    def take(n):
        return [next(it) for _ in range(n)]

    src, moments, out, new = take(3), take(6), take(3), take(6)
    buf, tmp, sem, bsem = take(4)
    copies = [pltpu.make_async_copy(x, y, sem.at[i]) for i, (x, y) in enumerate(zip(src[:2] + moments, out[:2] + new, strict=True))]
    for one in copies:
        one.start()

    def back(layer, x, n):
        return pltpu.make_async_copy(buf.at[n], out[2].at[layer, x], bsem.at[n])

    for layer in range(2):
        for x in range(4):
            n = 4 * layer + x

            @pl.loop(0, 3)
            def _(j):
                cols = pl.ds(pl.multiple_of(j * 256, 256), 256)
                for y in range(4):
                    for z in range(4):
                        tmp[28 * z : 28 * z + 28] = src[2][layer, z, x, 28 * y : 28 * y + 28, cols].astype(F32)
                    buf[n, y, :, cols] = tmp[...].astype(BF)

            back(layer, x, n).start()
    for layer in range(2):
        for x in range(4):
            back(layer, x, 4 * layer + x).wait()
    for one in copies:
        one.wait()


def solution(mesh):
    def step(*arrays):
        terms, weights, m, v = (arrays[i : i + 3] for i in (0, 3, 6, 9))
        whole = [(2, 4, 4, R[a], COLS[a]) for a in range(3)]
        terms = [t[0].reshape(s) for t, s in zip(terms, whole, strict=True)]
        views = [w.reshape(s) for w, s in zip(weights, whole, strict=True)]
        m, v = ([x.transpose(1, 0, 2) for x in y] for y in (m, v))
        vmem = pl.BlockSpec(memory_space=pltpu.VMEM)
        hbm = pl.BlockSpec(memory_space=pl.ANY)
        per = lambda fn, dt: [pltpu.VMEM(fn(a), dt) for a in range(3)]
        moment = lambda a: (H[a], 2, COLS[a])
        rows = lambda a: (2, 16, COLS[a])
        n = len(pairs())
        scratch = (
            per(lambda a: (4, 4, R[a], COLS[a]), BF) * 2
            + [pltpu.VMEM((4, 4, R[2], COLS[2]), F32)]
            + per(lambda a: (3, 4, R[a], COLS[a]), BF) * 2
            + per(lambda a: (4, R[a], COLS[a]), F32)
            + per(lambda a: (3, R[a], COLS[a]), BF) * 2
            + per(lambda a: (4, RP[a], COLS[a]), F32)
            + per(lambda a: (3, RP[a], COLS[a]), BF) * 2
            + per(rows, BF) * 4
            + per(lambda a: (4, RP[a], COLS[a]), BF)
            + per(lambda a: (2, R[a], COLS[a]), BF)
            + per(lambda a: (2, 8 if a < 2 else 16, COLS[a]), F32)
            + per(moment, F32) * 2
            + [pltpu.VMEM((4, 48, COLS[1]), BF), pltpu.VMEM((112, 256 * max(max(t) for t in TILES)), F32)]
            + [pltpu.SemaphoreType.DMA((n,)), pltpu.SemaphoreType.DMA((9,)), pltpu.SemaphoreType.DMA((n, 7)), pltpu.SemaphoreType.DMA((n, 17))]
        )
        got = pl.pallas_call(
            comm_kernel,
            out_shape=[pltpu.VMEM(s, BF) for s in whole] + per(moment, F32) * 2,
            in_specs=[hbm] * 12,
            out_specs=[vmem] * 9,
            scratch_shapes=scratch,
            compiler_params=pltpu.CompilerParams(collective_id=0, has_side_effects=True, vmem_limit_bytes=VMEM_LIMIT),
        )(*terms, *views, *m, *v)
        kept = [pltpu.with_memory_space_constraint(x, pltpu.VMEM) for x in got]
        done = pl.pallas_call(
            finish_kernel,
            out_shape=[jax.ShapeDtypeStruct(s, BF) for s in whole] + [jax.ShapeDtypeStruct(moment(a), F32) for a in range(3)] * 2,
            in_specs=[vmem] * 9,
            out_specs=[hbm] * 9,
            scratch_shapes=[
                pltpu.VMEM((8, 4, R[2], COLS[2]), BF),
                pltpu.VMEM((112, 256), F32),
                pltpu.SemaphoreType.DMA((8,)),
                pltpu.SemaphoreType.DMA((8,)),
            ],
            compiler_params=pltpu.CompilerParams(vmem_limit_bytes=20_000_000),
        )(*kept)
        return [x.reshape(w.shape) for x, w in zip(done[:3], weights, strict=True)] + [x.transpose(1, 0, 2) for x in done[3:]]

    def run(*arrays):
        return tuple(step(*arrays))

    all_of, cut = P(None, None, None), P(None, "dp", None)
    return jax.shard_map(
        run,
        mesh=mesh,
        in_specs=(P(("rep", "dp"), None, None, None),) * 3 + (all_of,) * 3 + (cut,) * 6,
        out_specs=(P("rep", None, None),) * 3 + (P("rep", "dp", None),) * 6,
        check_vma=False,
    )
```

```python
import jax
import jax.numpy as jnp
from jax import lax
from jax.experimental import pallas as pl
from jax.experimental.pallas import tpu as pltpu
from jax.sharding import PartitionSpec as P

MESH = pl.DeviceIdType.MESH
BF, F32 = jnp.bfloat16, jnp.float32

COLS = (1792, 1792, 768)
R = (48, 48, 112)
RC = (12, 12, 28)
RP = (16, 16, 32)
H = (6, 6, 14)
AXES = ((0, 1, 2), (1, 2, 0), (2, 0, 1))
TILES = ((1, 2, 2, 2), (1, 2, 2, 2), (1, 1, 1))
VMEM_LIMIT = 49_500_000
ORDER = (
    "aaeeiibbfjeafbigdfejjcbhaieddkbgfgkihecacjbfikh",
    "gedfbacijkhedgfcbakjhidgecbfkiahjedbeefcgaiikih",
    "jeebbdcfgahjdikacffgbhjjjfkabaacccghikadeiegjfe",
    "bbijjkahhcddhhkgggkdgcijffkachcdhfkdkdghjbckdg",
)
FIRST, PREPARE = 2, 18


def adamw(w, m, v, g):
    m = 0.9 * m + 0.1 * g
    v = 0.95 * v + 0.05 * g * g
    step = m * lax.rsqrt(v + 1e-8) + 0.1 * w
    return w - 0.02 * step, m, v


class Unit:
    def __init__(self, way, c0, cn):
        self.s, self.cn, self.cols = way, cn, pl.ds(c0, cn)


class Pair:
    def __init__(self, color, chunk, uid, c0, cn):
        self.a, self.chunk, self.p, self.cn, self.cols = color, chunk, uid, cn, pl.ds(c0, cn)
        self.units = (Unit(1, c0, cn // 2), Unit(-1, c0 + cn // 2, cn // 2))


def pairs():
    found = []
    for a in range(3):
        c0 = 0
        for k, t in enumerate(TILES[a]):
            found.append(Pair(a, k, len(found), c0, 256 * t))
            c0 += 256 * t
    return found


RECV = (0, 1, 2, 3, 4, 5, 6, 3, 0, 1, 2, 7, 8, 9, 10, 11, 12)
SEND = (0, 1, 2, 0, 1, 2, 3, 3, 0, 1, 2, 0, 1, 2, 4, 4, 5)


def comm_kernel(*refs):
    it = iter(refs)

    def take(n):
        return [next(it) for _ in range(n)]

    g, wh, mh, vh = take(3), take(3), take(3), take(3)
    out, mo, vo = take(3), take(3), take(3)
    own, part = take(3), take(3)
    psum = next(it)
    s1, r1, a1, s2, r2, a2, s3, r3 = (take(3) for _ in range(8))
    ag3, wz, wsel, msel, vsel, ms, vs, m, v, pm, pv = (take(3) for _ in range(11))
    ag2u, tmp, osem, msem, psem, qsem, ssem, rsem = take(8)
    all_pairs = pairs()

    me = lax.axis_index("dp")
    rep = lax.axis_index("rep")
    c = lax.rem(me, 2)
    pos = (me // 32, lax.rem(me // 8, 4), lax.rem(me // 2, 4))
    strides = (32, 8, 2)
    partner = me + 1 - 2 * c

    def near(axis, d):
        return me + (lax.rem(pos[axis] + d + 4, 4) - pos[axis]) * strides[axis]

    def message(u, i, src, dst, to):
        return pltpu.make_async_remote_copy(
            src_ref=src, dst_ref=dst, send_sem=ssem.at[u.p, SEND[i]], recv_sem=rsem.at[u.p, RECV[i]], device_id=(rep, to), device_id_type=MESH
        )

    leaving = {}

    def post(u, i, sends, whole):
        key = (u.p, SEND[i])
        if key in leaving and i != 16:
            leaving.pop(key)()
        for one in sends:
            message(u, i, *one).start()
        leaving[key] = lambda: message(u, i, whole, whole, partner).wait_send()

    def got(u, i, whole):
        message(u, i, whole, whole, partner).wait_recv()

    def loads(u):
        return pltpu.make_async_copy(g[u.a].at[c, :, :, :, u.cols], own[u.a].at[:, :, :, u.cols], osem.at[u.p])

    def mine1(u, cols, q, i):
        if u.a == 2:
            return psum[q, i, :, cols]
        where = (q, i) if u.a == 0 else (i, q)
        return own[u.a][(*where, slice(None), cols)].astype(F32) + part[u.a][(*where, slice(None), cols)].astype(F32)

    def mine2(u, cols, q, i):
        return a1[u.a][q, :, cols]

    def mine3(u, cols, q, i):
        return a2[u.a][q, :, cols]

    def axis(u, phase):
        return AXES[u.a][phase]

    def at(u, phase, d):
        return lax.rem(pos[axis(u, phase)] + d + 4, 4)

    mines, outs, ins = (mine1, mine2, mine3), (s1, s2, s3), (r1, r2, r3)

    def add(u, cols, phase, i, q):
        src, dst = ins[phase][u.a], outs[phase][u.a]
        if phase == 0:

            @pl.loop(0, 4)
            def _(j):
                x = mine1(u, cols, q, j)
                if i == 2:
                    x = x + src[0, j, :, cols].astype(F32)
                dst[i, j, :, cols] = x.astype(BF)

        else:
            x = mines[phase](u, cols, q, 0)
            if i == 2:
                x = x + src[0, :, cols].astype(F32)
            dst[i, :, cols] = x.astype(BF)

    def view(ref, phase, i, cols):
        return ref.at[i, :, :, cols] if phase == 0 else ref.at[i, :, cols]

    def give(u, phase, i):
        src, dst = outs[phase][u.a], ins[phase][u.a]
        if i == 0:
            add(u, u.cols, phase, 0, at(u, phase, 2))
        else:
            for t in u.units:
                add(u, t.cols, phase, i, at(u, phase, -t.s if i == 1 else t.s))
        sends = [(view(src, phase, i, t.cols), view(dst, phase, i, t.cols), near(axis(u, phase), -t.s if i == 1 else t.s)) for t in u.units]
        post(u, 3 * phase + i, sends, view(src, phase, i, u.cols))

    def give_all(u):
        sends = []
        for n, d in enumerate((2, 1, -1)):
            s3[u.a][n, :, u.cols] = a2[u.a][at(u, 2, d), :, u.cols].astype(BF)
            sends.append((s3[u.a].at[n, :, u.cols], r3[u.a].at[n, :, u.cols], near(axis(u, 2), d)))
        post(u, 6, sends, s3[u.a].at[:, :, u.cols])

    def take_in(u, phase, i):
        got(u, 3 * phase + i, view(ins[phase][u.a], phase, i, u.cols))

    def swap(u):
        post(u, 14, [(g[u.a].at[1 - c, :, :, :, u.cols], part[u.a].at[:, :, :, u.cols], partner)], part[u.a].at[:, :, :, u.cols])

    def st0(u):
        loads(u).wait()
        got(u, 14, part[u.a].at[:, :, :, u.cols])
        if u.a == 2:

            @pl.loop(0, 4)
            def _(x):
                for y in range(4):
                    t = own[2][x, y, :, u.cols].astype(F32) + part[2][x, y, :, u.cols].astype(F32)
                    for z in range(4):
                        psum[z, x, 28 * y : 28 * y + 28, u.cols] = t[28 * z : 28 * z + 28]

        give(u, 0, 0)

    def st1(u):
        give(u, 0, 1)

    def st2(u):
        take_in(u, 0, 0)
        give(u, 0, 2)

    def st3(u):
        take_in(u, 0, 1)
        take_in(u, 0, 2)
        q = pos[axis(u, 0)]

        def total(j):
            return mine1(u, u.cols, q, j) + r1[u.a][1, j, :, u.cols].astype(F32) + r1[u.a][2, j, :, u.cols].astype(F32)

        if u.a == 1:
            for j in range(4):
                t = total(j)
                for z in range(4):
                    a1[1][z, 12 * j : 12 * j + 12, u.cols] = t[12 * z : 12 * z + 12]
        else:

            @pl.loop(0, 4)
            def _(j):
                a1[u.a][j, :, u.cols] = total(j)

        give(u, 1, 0)
        give(u, 1, 1)

    def st4(u):
        take_in(u, 1, 0)
        give(u, 1, 2)

    def st5(u):
        take_in(u, 1, 1)
        take_in(u, 1, 2)
        rc = RC[u.a]
        t = a1[u.a][pos[axis(u, 1)], :, u.cols] + r2[u.a][1, :, u.cols].astype(F32) + r2[u.a][2, :, u.cols].astype(F32)
        for q in range(4):
            a2[u.a][q, 0:rc, u.cols] = t[rc * q : rc * q + rc]
        give_all(u)

    def st6(u):
        got(u, 6, r3[u.a].at[:, :, u.cols])
        h, rp = H[u.a], RP[u.a]
        t = a2[u.a][pos[axis(u, 2)], :, u.cols]
        for n in range(3):
            t = t + r3[u.a][n, :, u.cols].astype(F32)
        for q in range(2):
            grad = t[h * q : h * q + h].astype(BF).astype(F32)
            new, mn, vn = adamw(wsel[u.a][q, 0:h, u.cols], msel[u.a][q, 0:h, u.cols], vsel[u.a][q, 0:h, u.cols], grad)
            tmp[h * q : h * q + h, 0 : u.cn] = new
            ms[u.a][q, 0:h, u.cols] = mn
            vs[u.a][q, 0:h, u.cols] = vn
        ag3[u.a][pos[axis(u, 2)], :, u.cols] = tmp[0:rp, 0 : u.cn].astype(BF)
        block = ag3[u.a].at[pos[axis(u, 2)], :, u.cols]
        post(u, 7, [(block, block, near(axis(u, 2), d)) for d in (2, 1, -1)], ag3[u.a].at[0:3, :, u.cols])
        pairs_of = [(x[u.a].at[1 - c, :, u.cols], y[u.a].at[c, :, u.cols], partner) for x, y in ((ms, mo), (vs, vo))]
        post(u, 15, pairs_of, ms[u.a].at[:, :, u.cols])
        for x, y in ((ms, mo), (vs, vo)):
            y[u.a][c, 0:h, u.cols] = x[u.a][c, 0:h, u.cols]

    def ref2(u, cols):
        if u.a == 0:
            return lambda q: out[0].at[c, pos[0], q, :, cols]
        if u.a == 1:
            return lambda q: ag2u.at[q, :, cols]
        return lambda q: out[2].at[c, pos[2], q, :, cols]

    def ref1(u, cols, layer=c):
        if u.a == 1:
            return lambda q: out[1].at[layer, :, q, :, cols]
        return lambda q: out[u.a].at[layer, q, :, :, cols]

    refs_of = (ref1, ref2)

    def base(phase):
        return 11 - 3 * phase

    def spread(u, phase, i):
        sends = []
        for t in u.units:
            block = refs_of[phase](u, t.cols)(at(u, phase, -t.s) if i == 2 else pos[axis(u, phase)])
            sends.append((block, block, near(axis(u, phase), -t.s if i == 1 else t.s)))
        post(u, base(phase) + i, sends, refs_of[phase](u, u.cols)(pos[axis(u, phase)]))

    def arrived(u, phase, i):
        got(u, base(phase) + i, refs_of[phase](u, u.cols)(at(u, phase, 2)))

    def over(u, d):
        if d % 2 == 0:
            block = ref1(u, u.cols)(at(u, 0, d))
            sends = [(block, block, partner)]
        else:
            blocks = [ref1(u, t.cols)(at(u, 0, d * t.s)) for t in u.units]
            sends = [(x, x, partner) for x in blocks]
        post(u, 16, sends, out[u.a].at[c, :, :, :, u.cols])

    def st7(u):
        got(u, 7, ag3[u.a].at[0:3, :, u.cols])
        rc, r = RC[u.a], R[u.a]
        for q in range(4):
            tmp[rc * q : rc * q + rc, 0 : u.cn] = ag3[u.a][q, 0:rc, u.cols].astype(F32)
        ref2(u, u.cols)(pos[axis(u, 1)])[...] = tmp[0:r, 0 : u.cn].astype(BF)
        spread(u, 1, 0)
        spread(u, 1, 1)

    def st8(u):
        arrived(u, 1, 0)
        spread(u, 1, 2)

    def st9(u):
        arrived(u, 1, 1)
        arrived(u, 1, 2)
        if u.a == 1:
            for x in range(4):
                for z in range(4):
                    tmp[12 * z : 12 * z + 12, 0 : u.cn] = ag2u[z, 12 * x : 12 * x + 12, u.cols].astype(F32)
                out[1][c, x, pos[1], :, u.cols] = tmp[0:48, 0 : u.cn].astype(BF)
        spread(u, 0, 0)

    def st10(u):
        spread(u, 0, 1)

    def st11(u):
        over(u, 0)

    def st12(u):
        arrived(u, 0, 0)
        spread(u, 0, 2)

    def st13(u):
        over(u, -1)

    def st14(u):
        arrived(u, 0, 1)
        over(u, 1)

    def st15(u):
        arrived(u, 0, 2)
        over(u, 2)

    def st16(u):
        got(u, 15, mo[u.a].at[:, :, u.cols])
        got(u, 16, out[u.a].at[1 - c, :, :, :, u.cols])

    small, swaps = [], []
    for a in range(3):
        small.append((wh[a].at[c, pos[0], pos[1]], wz[a]))
        small.append((mh[a], m[a]))
        small.append((vh[a], v[a]))
        swaps.append((mh[a], pm[a]))
        swaps.append((vh[a], pv[a]))
    small = [pltpu.make_async_copy(src, dst, msem.at[n]) for n, (src, dst) in enumerate(small)]
    swaps = [
        pltpu.make_async_remote_copy(
            src_ref=src, dst_ref=dst, send_sem=psem.at[n], recv_sem=qsem.at[n], device_id=(rep, partner), device_id_type=MESH
        )
        for n, (src, dst) in enumerate(swaps)
    ]

    def prepare():
        for one in small:
            one.wait()
        for one in swaps:
            one.wait()
        for a in range(3):
            h = H[a]
            for src, theirs, dst in ((m, pm, msel), (v, pv, vsel)):
                dst[a][c, 0:h] = jnp.where(c == 0, src[a][:, 0], src[a][:, 1])
                dst[a][1 - c, 0:h] = jnp.where(c == 0, theirs[a][:, 0], theirs[a][:, 1])

            @pl.loop(0, COLS[a] // 256)
            def _(j):
                cols = pl.ds(pl.multiple_of(j * 256, 256), 256)
                line = wz[a][:, cols].astype(F32)
                for q in range(2):
                    rows = line[h * q : h * q + h]
                    for z in range(1, 4):
                        rows = jnp.where(pos[2] == z, line[h * (2 * z + q) : h * (2 * z + q) + h], rows)
                    wsel[a][q, 0:h, cols] = rows

    by_chunk = sorted(all_pairs, key=lambda u: ((u.chunk + 1) / len(TILES[u.a]), u.p))
    for u in by_chunk:
        loads(u).start()
    barrier = pltpu.get_barrier_semaphore()
    peers = [partner] + [near(x, d) for x in range(3) for d in (1, -1, 2)]
    for peer in peers:
        pl.semaphore_signal(barrier, inc=1, device_id=(rep, peer), device_id_type=MESH)
    pl.semaphore_wait(barrier, len(peers))

    for n, u in enumerate(by_chunk):
        swap(u)
        if n == FIRST:
            for one in swaps:
                one.start()
            for one in small:
                one.start()

    stages = (st0, st1, st2, st3, st4, st5, st6, st7, st8, st9, st10, st11, st12, st13, st14, st15, st16)
    done = [0] * len(all_pairs)
    for n, letter in enumerate("".join(ORDER)):
        p = "abcdefghijklmnop".index(letter)
        stages[done[p]](all_pairs[p])
        done[p] += 1
        if n == PREPARE:
            prepare()
    for wait in leaving.values():
        wait()


def finish_kernel(*refs):
    it = iter(refs)

    def take(n):
        return [next(it) for _ in range(n)]

    src, moments, out, new = take(3), take(6), take(3), take(6)
    buf, tmp, sem, bsem = take(4)
    turned = take(6)
    copies = [pltpu.make_async_copy(x, y, sem.at[i]) for i, (x, y) in enumerate(zip(src[:2] + turned, out[:2] + new, strict=True))]
    for one in copies[:2]:
        one.start()
    for n in range(6):
        for layer in range(2):
            turned[n][:, layer] = moments[n][layer, 0 : H[n % 3]]
        copies[2 + n].start()

    def back(layer, x, n):
        return pltpu.make_async_copy(buf.at[n], out[2].at[layer, x], bsem.at[n])

    for layer in range(2):
        for x in range(4):
            n = 4 * layer + x

            @pl.loop(0, 3)
            def _(j):
                cols = pl.ds(pl.multiple_of(j * 256, 256), 256)
                for y in range(4):
                    for z in range(4):
                        tmp[28 * z : 28 * z + 28] = src[2][layer, z, x, 28 * y : 28 * y + 28, cols].astype(F32)
                    buf[n, y, :, cols] = tmp[...].astype(BF)

            back(layer, x, n).start()
    for layer in range(2):
        for x in range(4):
            back(layer, x, 4 * layer + x).wait()
    for one in copies:
        one.wait()


def solution(mesh):
    def step(*arrays):
        terms, weights, m, v = (arrays[i : i + 3] for i in (0, 3, 6, 9))
        whole = [(2, 4, 4, R[a], COLS[a]) for a in range(3)]
        terms = [t[0].reshape(s) for t, s in zip(terms, whole, strict=True)]
        views = [w.reshape(s) for w, s in zip(weights, whole, strict=True)]
        m, v = ([x.transpose(1, 0, 2) for x in y] for y in (m, v))
        vmem = pl.BlockSpec(memory_space=pltpu.VMEM)
        hbm = pl.BlockSpec(memory_space=pl.ANY)
        per = lambda fn, dt: [pltpu.VMEM(fn(a), dt) for a in range(3)]
        moment = lambda a: (H[a], 2, COLS[a])
        rows = lambda a: (2, 8 if a < 2 else 16, COLS[a])
        n = len(pairs())
        scratch = (
            per(lambda a: (4, 4, R[a], COLS[a]), BF) * 2
            + [pltpu.VMEM((4, 4, R[2], COLS[2]), F32)]
            + per(lambda a: (3, 4, R[a], COLS[a]), BF) * 2
            + per(lambda a: (4, R[a], COLS[a]), F32)
            + per(lambda a: (3, R[a], COLS[a]), BF) * 2
            + per(lambda a: (4, RP[a], COLS[a]), F32)
            + per(lambda a: (3, RP[a], COLS[a]), BF) * 2
            + per(lambda a: (4, RP[a], COLS[a]), BF)
            + per(lambda a: (R[a], COLS[a]), BF)
            + per(rows, F32) * 5
            + per(moment, F32) * 4
            + [pltpu.VMEM((4, 48, COLS[1]), BF), pltpu.VMEM((112, 256 * max(max(t) for t in TILES)), F32)]
            + [pltpu.SemaphoreType.DMA((k,)) for k in (n, 9, 6, 6)]
            + [pltpu.SemaphoreType.DMA((n, max(SEND) + 1)), pltpu.SemaphoreType.DMA((n, max(RECV) + 1))]
        )
        got = pl.pallas_call(
            comm_kernel,
            out_shape=[pltpu.VMEM(s, BF) for s in whole] + per(rows, F32) * 2,
            in_specs=[hbm] * 12,
            out_specs=[vmem] * 9,
            scratch_shapes=scratch,
            compiler_params=pltpu.CompilerParams(collective_id=0, has_side_effects=True, vmem_limit_bytes=VMEM_LIMIT),
        )(*terms, *views, *m, *v)
        kept = [pltpu.with_memory_space_constraint(x, pltpu.VMEM) for x in got]
        done = pl.pallas_call(
            finish_kernel,
            out_shape=[jax.ShapeDtypeStruct(s, BF) for s in whole] + [jax.ShapeDtypeStruct(moment(a), F32) for a in range(3)] * 2,
            in_specs=[vmem] * 9,
            out_specs=[hbm] * 9,
            scratch_shapes=[
                pltpu.VMEM((8, 4, R[2], COLS[2]), BF),
                pltpu.VMEM((112, 256), F32),
                pltpu.SemaphoreType.DMA((8,)),
                pltpu.SemaphoreType.DMA((8,)),
            ]
            + per(moment, F32) * 2,
            compiler_params=pltpu.CompilerParams(vmem_limit_bytes=20_000_000),
        )(*kept)
        return [x.reshape(w.shape) for x, w in zip(done[:3], weights, strict=True)] + [x.transpose(1, 0, 2) for x in done[3:]]

    def run(*arrays):
        return tuple(step(*arrays))

    all_of, cut = P(None, None, None), P(None, "dp", None)
    return jax.shard_map(
        run,
        mesh=mesh,
        in_specs=(P(("rep", "dp"), None, None, None),) * 3 + (all_of,) * 3 + (cut,) * 6,
        out_specs=(P("rep", None, None),) * 3 + (P("rep", "dp", None),) * 6,
        check_vma=False,
    )
```

```python
import jax
import jax.numpy as jnp
from jax import lax
from jax.experimental import pallas as pl
from jax.experimental.pallas import tpu as pltpu
from jax.sharding import PartitionSpec as P

MESH = pl.DeviceIdType.MESH
BF, F32 = jnp.bfloat16, jnp.float32

COLS = (1792, 1792, 768)
R = (48, 48, 112)
RC = (12, 12, 28)
RP = (16, 16, 32)
H = (6, 6, 14)
AXES = ((0, 1, 2), (1, 2, 0), (2, 0, 1))
TILES = ((1, 2, 2, 2), (1, 2, 2, 2), (1, 1, 1))
VMEM_LIMIT = 49_500_000
ORDER = (
    "aaeeiibbfjeafbigdfejjcbhaieddkbgfgkihecacjbfikh",
    "gedfbacijkhedgfcbakjhidgecbfkiahjedbeefcgaiikih",
    "jeebbdcfgahjdikacffgbhjjjfkabaacccghikadeiegjfe",
    "bbijjkahhcddhhkgggkdgcijffkachcdhfkdkdghjbckdg",
)
FIRST, PREPARE = 5, 30


def adamw(w, m, v, g):
    m = 0.9 * m + 0.1 * g
    v = 0.95 * v + 0.05 * g * g
    step = m * lax.rsqrt(v + 1e-8) + 0.1 * w
    return w - 0.02 * step, m, v


class Unit:
    def __init__(self, way, c0, cn):
        self.s, self.cn, self.cols = way, cn, pl.ds(c0, cn)


class Pair:
    def __init__(self, color, chunk, uid, c0, cn):
        self.a, self.chunk, self.p, self.cn, self.cols = color, chunk, uid, cn, pl.ds(c0, cn)
        self.units = (Unit(1, c0, cn // 2), Unit(-1, c0 + cn // 2, cn // 2))


def pairs():
    found = []
    for a in range(3):
        c0 = 0
        for k, t in enumerate(TILES[a]):
            found.append(Pair(a, k, len(found), c0, 256 * t))
            c0 += 256 * t
    return found


RECV = (0, 1, 1, 2, 3, 3, 4, 2, 0, 1, 1, 5, 6, 7, 8, 9, 10)
SEND = (0, 0, 0, 1, 1, 1, 2, 2, 0, 0, 0, 1, 1, 1, 3, 3, 4)
SAME = [range(i - i % 3, i - i % 3 + 3) if i < 6 else range(i - (i + 1) % 3, i - (i + 1) % 3 + 3) if 8 <= i < 14 else (i,) for i in range(17)]


def comm_kernel(*refs):
    it = iter(refs)

    def take(n):
        return [next(it) for _ in range(n)]

    g, wh, mh, vh = take(3), take(3), take(3), take(3)
    out, mo, vo = take(3), take(3), take(3)
    own, part = take(3), take(3)
    psum = next(it)
    s1, r1, a1, s2, r2, a2, s3, r3 = (take(3) for _ in range(8))
    ag3, wz, wsel, msel, vsel, ms, vs, m, v, pm, pv = (take(3) for _ in range(11))
    ag2u, tmp, osem, msem, psem, qsem, ssem, rsem = take(8)
    all_pairs = pairs()

    me = lax.axis_index("dp")
    rep = lax.axis_index("rep")
    c = lax.rem(me, 2)
    pos = (me // 32, lax.rem(me // 8, 4), lax.rem(me // 2, 4))
    strides = (32, 8, 2)
    partner = me + 1 - 2 * c

    ahead = [[lax.rem(pos[x] + d, 4) for d in range(4)] for x in range(3)]
    nearby = [[me + (ahead[x][d] - pos[x]) * strides[x] for d in range(4)] for x in range(3)]

    def near(axis, d):
        return nearby[axis][d % 4]

    def message(u, i, src, dst, to):
        return pltpu.make_async_remote_copy(
            src_ref=src, dst_ref=dst, send_sem=ssem.at[u.p, SEND[i]], recv_sem=rsem.at[u.p, RECV[i]], device_id=(rep, to), device_id_type=MESH
        )

    leaving = {}

    def post(u, i, sends, whole):
        key = (u.p, SEND[i])
        if key in leaving and leaving[key][0] not in SAME[i]:
            leaving.pop(key)[1]()
        for one in sends:
            message(u, i, *one).start()
        leaving[key] = i, lambda: message(u, i, whole, whole, partner).wait_send()

    def got(u, i, whole):
        message(u, i, whole, whole, partner).wait_recv()

    def loads(u):
        return pltpu.make_async_copy(g[u.a].at[c, :, :, :, u.cols], own[u.a].at[:, :, :, u.cols], osem.at[u.p])

    def mine1(u, cols, q, i):
        if u.a == 2:
            return psum[q, i, :, cols]
        where = (q, i) if u.a == 0 else (i, q)
        return own[u.a][(*where, slice(None), cols)].astype(F32) + part[u.a][(*where, slice(None), cols)].astype(F32)

    def mine2(u, cols, q, i):
        return a1[u.a][q, :, cols]

    def mine3(u, cols, q, i):
        return a2[u.a][q, :, cols]

    def axis(u, phase):
        return AXES[u.a][phase]

    def at(u, phase, d):
        return ahead[axis(u, phase)][d % 4]

    mines, outs, ins = (mine1, mine2, mine3), (s1, s2, s3), (r1, r2, r3)

    def add(u, cols, phase, i, q):
        src, dst = ins[phase][u.a], outs[phase][u.a]
        if phase == 0:

            @pl.loop(0, 4)
            def _(j):
                x = mine1(u, cols, q, j)
                if i == 2:
                    x = x + src[0, j, :, cols].astype(F32)
                dst[i, j, :, cols] = x.astype(BF)

        else:
            x = mines[phase](u, cols, q, 0)
            if i == 2:
                x = x + src[0, :, cols].astype(F32)
            dst[i, :, cols] = x.astype(BF)

    def view(ref, phase, i, cols):
        return ref.at[i, :, :, cols] if phase == 0 else ref.at[i, :, cols]


    def give(u, phase, i):
        src, dst = outs[phase][u.a], ins[phase][u.a]
        if i == 0:
            add(u, u.cols, phase, 0, at(u, phase, 2))
        else:
            for t in u.units:
                add(u, t.cols, phase, i, at(u, phase, -t.s if i == 1 else t.s))
        sends = [(view(src, phase, i, t.cols), view(dst, phase, i, t.cols), near(axis(u, phase), -t.s if i == 1 else t.s)) for t in u.units]
        post(u, 3 * phase + i, sends, view(src, phase, slice(None), u.cols))

    def give_all(u):
        sends = []
        for n, d in enumerate((2, 1, -1)):
            s3[u.a][n, :, u.cols] = a2[u.a][at(u, 2, d), :, u.cols].astype(BF)
            sends.append((s3[u.a].at[n, :, u.cols], r3[u.a].at[n, :, u.cols], near(axis(u, 2), d)))
        post(u, 6, sends, s3[u.a].at[:, :, u.cols])

    def take_in(u, phase, i):
        got(u, 3 * phase + i, view(ins[phase][u.a], phase, i, u.cols))

    def swap(u):
        post(u, 14, [(g[u.a].at[1 - c, :, :, :, u.cols], part[u.a].at[:, :, :, u.cols], partner)], part[u.a].at[:, :, :, u.cols])

    def st0(u):
        loads(u).wait()
        got(u, 14, part[u.a].at[:, :, :, u.cols])
        if u.a == 2:

            @pl.loop(0, 4)
            def _(x):
                for y in range(4):
                    t = own[2][x, y, :, u.cols].astype(F32) + part[2][x, y, :, u.cols].astype(F32)
                    for z in range(4):
                        psum[z, x, 28 * y : 28 * y + 28, u.cols] = t[28 * z : 28 * z + 28]

        give(u, 0, 0)

    def st1(u):
        give(u, 0, 1)

    def st2(u):
        take_in(u, 0, 0)
        give(u, 0, 2)

    def st3(u):
        got(u, 1, view(r1[u.a], 0, slice(1, 3), u.cols))
        q = pos[axis(u, 0)]

        def total(j):
            return mine1(u, u.cols, q, j) + r1[u.a][1, j, :, u.cols].astype(F32) + r1[u.a][2, j, :, u.cols].astype(F32)

        if u.a == 1:
            for j in range(4):
                t = total(j)
                for z in range(4):
                    a1[1][z, 12 * j : 12 * j + 12, u.cols] = t[12 * z : 12 * z + 12]
        else:

            @pl.loop(0, 4)
            def _(j):
                a1[u.a][j, :, u.cols] = total(j)

        give(u, 1, 0)
        give(u, 1, 1)

    def st4(u):
        take_in(u, 1, 0)
        give(u, 1, 2)

    def st5(u):
        got(u, 4, view(r2[u.a], 1, slice(1, 3), u.cols))
        rc = RC[u.a]
        t = a1[u.a][pos[axis(u, 1)], :, u.cols] + r2[u.a][1, :, u.cols].astype(F32) + r2[u.a][2, :, u.cols].astype(F32)
        for q in range(4):
            a2[u.a][q, 0:rc, u.cols] = t[rc * q : rc * q + rc]
        give_all(u)

    def st6(u):
        got(u, 6, r3[u.a].at[:, :, u.cols])
        h, rp = H[u.a], RP[u.a]
        t = a2[u.a][pos[axis(u, 2)], :, u.cols]
        for n in range(3):
            t = t + r3[u.a][n, :, u.cols].astype(F32)
        for q in range(2):
            grad = t[h * q : h * q + h].astype(BF).astype(F32)
            new, mn, vn = adamw(wsel[u.a][q, 0:h, u.cols], msel[u.a][q, 0:h, u.cols], vsel[u.a][q, 0:h, u.cols], grad)
            tmp[h * q : h * q + h, 0 : u.cn] = new
            ms[u.a][q, 0:h, u.cols] = mn
            vs[u.a][q, 0:h, u.cols] = vn
        ag3[u.a][pos[axis(u, 2)], :, u.cols] = tmp[0:rp, 0 : u.cn].astype(BF)
        block = ag3[u.a].at[pos[axis(u, 2)], :, u.cols]
        post(u, 7, [(block, block, near(axis(u, 2), d)) for d in (2, 1, -1)], ag3[u.a].at[0:3, :, u.cols])
        pairs_of = [(x[u.a].at[1 - c, :, u.cols], y[u.a].at[c, :, u.cols], partner) for x, y in ((ms, mo), (vs, vo))]
        post(u, 15, pairs_of, ms[u.a].at[:, :, u.cols])
        for x, y in ((ms, mo), (vs, vo)):
            y[u.a][c, 0:h, u.cols] = x[u.a][c, 0:h, u.cols]

    def ref2(u, cols):
        if u.a == 0:
            return lambda q: out[0].at[c, pos[0], q, :, cols]
        if u.a == 1:
            return lambda q: ag2u.at[q, :, cols]
        return lambda q: out[2].at[c, pos[2], q, :, cols]

    def ref1(u, cols, layer=c):
        if u.a == 1:
            return lambda q: out[1].at[layer, :, q, :, cols]
        return lambda q: out[u.a].at[layer, q, :, :, cols]

    refs_of = (ref1, ref2)

    def base(phase):
        return 11 - 3 * phase

    def spread(u, phase, i):
        sends = []
        for t in u.units:
            block = refs_of[phase](u, t.cols)(at(u, phase, -t.s) if i == 2 else pos[axis(u, phase)])
            sends.append((block, block, near(axis(u, phase), -t.s if i == 1 else t.s)))
        post(u, base(phase) + i, sends, thrice(u, phase))

    def arrived(u, phase, i):
        got(u, base(phase) + i, refs_of[phase](u, u.cols)(at(u, phase, 2)))

    def thrice(u, phase):
        return out[u.a].at[c, 0:3, :, :, u.cols] if phase == 0 else out[u.a].at[c, 0, 0:3, :, u.cols]

    def over(u, d):
        if d % 2 == 0:
            block = ref1(u, u.cols)(at(u, 0, d))
            sends = [(block, block, partner)]
        else:
            blocks = [ref1(u, t.cols)(at(u, 0, d * t.s)) for t in u.units]
            sends = [(x, x, partner) for x in blocks]
        post(u, 16, sends, out[u.a].at[c, :, :, :, u.cols])

    def st7(u):
        got(u, 7, ag3[u.a].at[0:3, :, u.cols])
        rc, r = RC[u.a], R[u.a]
        for q in range(4):
            tmp[rc * q : rc * q + rc, 0 : u.cn] = ag3[u.a][q, 0:rc, u.cols].astype(F32)
        ref2(u, u.cols)(pos[axis(u, 1)])[...] = tmp[0:r, 0 : u.cn].astype(BF)
        spread(u, 1, 0)
        spread(u, 1, 1)

    def st8(u):
        arrived(u, 1, 0)
        spread(u, 1, 2)

    def st9(u):
        got(u, 9, out[u.a].at[c, 0, 0:2, :, u.cols])
        if u.a == 1:
            for x in range(4):
                for z in range(4):
                    tmp[12 * z : 12 * z + 12, 0 : u.cn] = ag2u[z, 12 * x : 12 * x + 12, u.cols].astype(F32)
                out[1][c, x, pos[1], :, u.cols] = tmp[0:48, 0 : u.cn].astype(BF)
        spread(u, 0, 0)

    def st10(u):
        spread(u, 0, 1)

    def st11(u):
        over(u, 0)

    def st12(u):
        arrived(u, 0, 0)
        spread(u, 0, 2)

    def st13(u):
        over(u, -1)

    def st14(u):
        arrived(u, 0, 1)
        over(u, 1)

    def st15(u):
        arrived(u, 0, 2)
        over(u, 2)

    def st16(u):
        got(u, 15, mo[u.a].at[:, :, u.cols])
        got(u, 16, out[u.a].at[1 - c, :, :, :, u.cols])

    small, swaps = [], []
    for a in range(3):
        small.append((wh[a].at[c, pos[0], pos[1]], wz[a]))
        small.append((mh[a], m[a]))
        small.append((vh[a], v[a]))
        swaps.append((mh[a], pm[a]))
        swaps.append((vh[a], pv[a]))
    small = [pltpu.make_async_copy(src, dst, msem.at[n]) for n, (src, dst) in enumerate(small)]
    swaps = [
        pltpu.make_async_remote_copy(
            src_ref=src, dst_ref=dst, send_sem=psem.at[n], recv_sem=qsem.at[n], device_id=(rep, partner), device_id_type=MESH
        )
        for n, (src, dst) in enumerate(swaps)
    ]

    def prepare():
        for one in small:
            one.wait()
        for one in swaps:
            one.wait()
        for a in range(3):
            h = H[a]
            for src, theirs, dst in ((m, pm, msel), (v, pv, vsel)):
                dst[a][c, 0:h] = jnp.where(c == 0, src[a][:, 0], src[a][:, 1])
                dst[a][1 - c, 0:h] = jnp.where(c == 0, theirs[a][:, 0], theirs[a][:, 1])

            @pl.loop(0, COLS[a] // 256)
            def _(j):
                cols = pl.ds(pl.multiple_of(j * 256, 256), 256)
                line = wz[a][:, cols].astype(F32)
                for q in range(2):
                    rows = line[h * q : h * q + h]
                    for z in range(1, 4):
                        rows = jnp.where(pos[2] == z, line[h * (2 * z + q) : h * (2 * z + q) + h], rows)
                    wsel[a][q, 0:h, cols] = rows

    by_chunk = sorted(all_pairs, key=lambda u: ((u.chunk + 1) / len(TILES[u.a]), u.p))
    for u in by_chunk:
        loads(u).start()
    barrier = pltpu.get_barrier_semaphore()
    peers = [partner] + [near(x, d) for x in range(3) for d in (1, -1, 2)]
    for peer in peers:
        pl.semaphore_signal(barrier, inc=1, device_id=(rep, peer), device_id_type=MESH)
    pl.semaphore_wait(barrier, len(peers))

    for n, u in enumerate(by_chunk):
        swap(u)
        if n == FIRST:
            for one in swaps:
                one.start()
            for one in small:
                one.start()

    stages = (st0, st1, st2, st3, st4, st5, st6, st7, st8, st9, st10, st11, st12, st13, st14, st15, st16)
    done = [0] * len(all_pairs)
    for n, letter in enumerate("".join(ORDER)):
        p = "abcdefghijklmnop".index(letter)
        stages[done[p]](all_pairs[p])
        done[p] += 1
        if n == PREPARE:
            prepare()
    for _, wait in leaving.values():
        wait()


def finish_kernel(*refs):
    it = iter(refs)

    def take(n):
        return [next(it) for _ in range(n)]

    src, moments, out, new = take(3), take(6), take(3), take(6)
    buf, tmp, sem, bsem = take(4)
    turned = take(6)
    copies = [pltpu.make_async_copy(x, y, sem.at[i]) for i, (x, y) in enumerate(zip(src[:2] + turned, out[:2] + new, strict=True))]
    for one in copies[:2]:
        one.start()
    for n in range(6):
        for layer in range(2):
            turned[n][:, layer] = moments[n][layer, 0 : H[n % 3]]
        copies[2 + n].start()

    def back(layer, x, n):
        return pltpu.make_async_copy(buf.at[n], out[2].at[layer, x], bsem.at[n])

    for layer in range(2):
        for x in range(4):
            n = 4 * layer + x

            @pl.loop(0, 3)
            def _(j):
                cols = pl.ds(pl.multiple_of(j * 256, 256), 256)
                for y in range(4):
                    for z in range(4):
                        tmp[28 * z : 28 * z + 28] = src[2][layer, z, x, 28 * y : 28 * y + 28, cols].astype(F32)
                    buf[n, y, :, cols] = tmp[...].astype(BF)

            back(layer, x, n).start()
    for layer in range(2):
        for x in range(4):
            back(layer, x, 4 * layer + x).wait()
    for one in copies:
        one.wait()


def solution(mesh):
    def step(*arrays):
        terms, weights, m, v = (arrays[i : i + 3] for i in (0, 3, 6, 9))
        whole = [(2, 4, 4, R[a], COLS[a]) for a in range(3)]
        terms = [t[0].reshape(s) for t, s in zip(terms, whole, strict=True)]
        views = [w.reshape(s) for w, s in zip(weights, whole, strict=True)]
        m, v = ([x.transpose(1, 0, 2) for x in y] for y in (m, v))
        vmem = pl.BlockSpec(memory_space=pltpu.VMEM)
        hbm = pl.BlockSpec(memory_space=pl.ANY)
        per = lambda fn, dt: [pltpu.VMEM(fn(a), dt) for a in range(3)]
        moment = lambda a: (H[a], 2, COLS[a])
        rows = lambda a: (2, 8 if a < 2 else 16, COLS[a])
        n = len(pairs())
        scratch = (
            per(lambda a: (4, 4, R[a], COLS[a]), BF) * 2
            + [pltpu.VMEM((4, 4, R[2], COLS[2]), F32)]
            + per(lambda a: (3, 4, R[a], COLS[a]), BF) * 2
            + per(lambda a: (4, R[a], COLS[a]), F32)
            + per(lambda a: (3, R[a], COLS[a]), BF) * 2
            + per(lambda a: (4, RP[a], COLS[a]), F32)
            + per(lambda a: (3, RP[a], COLS[a]), BF) * 2
            + per(lambda a: (4, RP[a], COLS[a]), BF)
            + per(lambda a: (R[a], COLS[a]), BF)
            + per(rows, F32) * 5
            + per(moment, F32) * 4
            + [pltpu.VMEM((4, 48, COLS[1]), BF), pltpu.VMEM((112, 256 * max(max(t) for t in TILES)), F32)]
            + [pltpu.SemaphoreType.DMA((k,)) for k in (n, 9, 6, 6)]
            + [pltpu.SemaphoreType.DMA((n, max(SEND) + 1)), pltpu.SemaphoreType.DMA((n, max(RECV) + 1))]
        )
        got = pl.pallas_call(
            comm_kernel,
            out_shape=[pltpu.VMEM(s, BF) for s in whole] + per(rows, F32) * 2,
            in_specs=[hbm] * 12,
            out_specs=[vmem] * 9,
            scratch_shapes=scratch,
            compiler_params=pltpu.CompilerParams(collective_id=0, has_side_effects=True, vmem_limit_bytes=VMEM_LIMIT),
        )(*terms, *views, *m, *v)
        kept = [pltpu.with_memory_space_constraint(x, pltpu.VMEM) for x in got]
        done = pl.pallas_call(
            finish_kernel,
            out_shape=[jax.ShapeDtypeStruct(s, BF) for s in whole] + [jax.ShapeDtypeStruct(moment(a), F32) for a in range(3)] * 2,
            in_specs=[vmem] * 9,
            out_specs=[hbm] * 9,
            scratch_shapes=[
                pltpu.VMEM((8, 4, R[2], COLS[2]), BF),
                pltpu.VMEM((112, 256), F32),
                pltpu.SemaphoreType.DMA((8,)),
                pltpu.SemaphoreType.DMA((8,)),
            ]
            + per(moment, F32) * 2,
            compiler_params=pltpu.CompilerParams(vmem_limit_bytes=20_000_000),
        )(*kept)
        return [x.reshape(w.shape) for x, w in zip(done[:3], weights, strict=True)] + [x.transpose(1, 0, 2) for x in done[3:]]

    def run(*arrays):
        return tuple(step(*arrays))

    all_of, cut = P(None, None, None), P(None, "dp", None)
    return jax.shard_map(
        run,
        mesh=mesh,
        in_specs=(P(("rep", "dp"), None, None, None),) * 3 + (all_of,) * 3 + (cut,) * 6,
        out_specs=(P("rep", None, None),) * 3 + (P("rep", "dp", None),) * 6,
        check_vma=False,
    )
```

```python
import jax
import jax.numpy as jnp
from jax import lax
from jax.experimental import pallas as pl
from jax.experimental.pallas import tpu as pltpu
from jax.sharding import PartitionSpec as P

MESH = pl.DeviceIdType.MESH
BF, F32 = jnp.bfloat16, jnp.float32

COLS = (1792, 1792, 768)
R = (48, 48, 112)
RC = (12, 12, 28)
RP = (16, 16, 32)
H = (6, 6, 14)
AXES = ((0, 1, 2), (1, 2, 0), (2, 0, 1))
TILES = ((1, 1, 1, 2, 2), (1, 1, 1, 2, 2), (1, 1, 1))
VMEM_LIMIT = 49_500_000
ORDER = (
    "aaffkkbggcahhflbddkgahljjedbalikhgejfmdkeighmcbcfdkamihl",
    "bgedcfajhlkmiebgdajcfhilmkebcajdhfimkglaebachfjdgkhhikml",
    "aafcekdajgibggklfmhhdjcgbigelflffmdglkhdjcaciimiemafbbmc",
    "cllafgbjckkijeeemibibdddhecjjcjgkblldehfimmmejibclemj",
)
FIRST, PREPARE = 6, 34


def adamw(w, m, v, g):
    m = 0.9 * m + 0.1 * g
    v = 0.95 * v + 0.05 * g * g
    step = m * lax.rsqrt(v + 1e-8) + 0.1 * w
    return w - 0.02 * step, m, v


class Unit:
    def __init__(self, way, c0, cn):
        self.s, self.cn, self.cols = way, cn, pl.ds(c0, cn)


class Pair:
    def __init__(self, color, chunk, uid, c0, cn):
        self.a, self.chunk, self.p, self.cn, self.cols = color, chunk, uid, cn, pl.ds(c0, cn)
        self.units = (Unit(1, c0, cn // 2), Unit(-1, c0 + cn // 2, cn // 2))


def pairs():
    found = []
    for a in range(3):
        c0 = 0
        for k, t in enumerate(TILES[a]):
            found.append(Pair(a, k, len(found), c0, 256 * t))
            c0 += 256 * t
    return found


RECV = (0, 1, 1, 2, 3, 3, 4, 2, 0, 1, 1, 5, 6, 7, 8, 9, 10)
SEND = (0, 0, 0, 1, 1, 1, 2, 2, 0, 0, 0, 1, 1, 1, 3, 3, 4)
SAME = [range(i - i % 3, i - i % 3 + 3) if i < 6 else range(i - (i + 1) % 3, i - (i + 1) % 3 + 3) if 8 <= i < 14 else (i,) for i in range(17)]


def comm_kernel(*refs):
    it = iter(refs)

    def take(n):
        return [next(it) for _ in range(n)]

    g, wh, mh, vh = take(3), take(3), take(3), take(3)
    out, mo, vo = take(3), take(3), take(3)
    own, part = take(3), take(3)
    psum = next(it)
    s1, r1, a1, s2, r2, a2, s3, r3 = (take(3) for _ in range(8))
    ag3, wz, wsel, msel, vsel, ms, vs, m, v, pm, pv = (take(3) for _ in range(11))
    ag2u, tmp, osem, msem, psem, qsem, ssem, rsem = take(8)
    all_pairs = pairs()

    me = lax.axis_index("dp")
    rep = lax.axis_index("rep")
    c = lax.rem(me, 2)
    pos = (me // 32, lax.rem(me // 8, 4), lax.rem(me // 2, 4))
    strides = (32, 8, 2)
    partner = me + 1 - 2 * c

    ahead = [[lax.rem(pos[x] + d, 4) for d in range(4)] for x in range(3)]
    nearby = [[me + (ahead[x][d] - pos[x]) * strides[x] for d in range(4)] for x in range(3)]

    def near(axis, d):
        return nearby[axis][d % 4]

    def message(u, i, src, dst, to):
        return pltpu.make_async_remote_copy(
            src_ref=src, dst_ref=dst, send_sem=ssem.at[u.p, SEND[i]], recv_sem=rsem.at[u.p, RECV[i]], device_id=(rep, to), device_id_type=MESH
        )

    leaving = {}

    def post(u, i, sends, whole):
        key = (u.p, SEND[i])
        if key in leaving and leaving[key][0] not in SAME[i]:
            leaving.pop(key)[1]()
        for one in sends:
            message(u, i, *one).start()
        leaving[key] = i, lambda: message(u, i, whole, whole, partner).wait_send()

    def got(u, i, whole):
        message(u, i, whole, whole, partner).wait_recv()

    def loads(u):
        return pltpu.make_async_copy(g[u.a].at[c, :, :, :, u.cols], own[u.a].at[:, :, :, u.cols], osem.at[u.p])

    def mine1(u, cols, q, i):
        if u.a == 2:
            return psum[q, i, :, cols]
        where = (q, i) if u.a == 0 else (i, q)
        return own[u.a][(*where, slice(None), cols)].astype(F32) + part[u.a][(*where, slice(None), cols)].astype(F32)

    def mine2(u, cols, q, i):
        return a1[u.a][q, :, cols]

    def mine3(u, cols, q, i):
        return a2[u.a][q, :, cols]

    def axis(u, phase):
        return AXES[u.a][phase]

    def at(u, phase, d):
        return ahead[axis(u, phase)][d % 4]

    mines, outs, ins = (mine1, mine2, mine3), (s1, s2, s3), (r1, r2, r3)

    def add(u, cols, phase, i, q):
        src, dst = ins[phase][u.a], outs[phase][u.a]
        if phase == 0:

            @pl.loop(0, 4)
            def _(j):
                x = mine1(u, cols, q, j)
                if i == 2:
                    x = x + src[0, j, :, cols].astype(F32)
                dst[i, j, :, cols] = x.astype(BF)

        else:
            x = mines[phase](u, cols, q, 0)
            if i == 2:
                x = x + src[0, :, cols].astype(F32)
            dst[i, :, cols] = x.astype(BF)

    def view(ref, phase, i, cols):
        return ref.at[i, :, :, cols] if phase == 0 else ref.at[i, :, cols]


    def give(u, phase, i):
        src, dst = outs[phase][u.a], ins[phase][u.a]
        if i == 0:
            add(u, u.cols, phase, 0, at(u, phase, 2))
        else:
            for t in u.units:
                add(u, t.cols, phase, i, at(u, phase, -t.s if i == 1 else t.s))
        sends = [(view(src, phase, i, t.cols), view(dst, phase, i, t.cols), near(axis(u, phase), -t.s if i == 1 else t.s)) for t in u.units]
        post(u, 3 * phase + i, sends, view(src, phase, slice(None), u.cols))

    def give_all(u):
        sends = []
        for n, d in enumerate((2, 1, -1)):
            s3[u.a][n, :, u.cols] = a2[u.a][at(u, 2, d), :, u.cols].astype(BF)
            sends.append((s3[u.a].at[n, :, u.cols], r3[u.a].at[n, :, u.cols], near(axis(u, 2), d)))
        post(u, 6, sends, s3[u.a].at[:, :, u.cols])

    def take_in(u, phase, i):
        got(u, 3 * phase + i, view(ins[phase][u.a], phase, i, u.cols))

    def swap(u):
        post(u, 14, [(g[u.a].at[1 - c, :, :, :, u.cols], part[u.a].at[:, :, :, u.cols], partner)], part[u.a].at[:, :, :, u.cols])

    def st0(u):
        loads(u).wait()
        got(u, 14, part[u.a].at[:, :, :, u.cols])
        if u.a == 2:

            @pl.loop(0, 4)
            def _(x):
                for y in range(4):
                    t = own[2][x, y, :, u.cols].astype(F32) + part[2][x, y, :, u.cols].astype(F32)
                    for z in range(4):
                        psum[z, x, 28 * y : 28 * y + 28, u.cols] = t[28 * z : 28 * z + 28]

        give(u, 0, 0)

    def st1(u):
        give(u, 0, 1)

    def st2(u):
        take_in(u, 0, 0)
        give(u, 0, 2)

    def st3(u):
        got(u, 1, view(r1[u.a], 0, slice(1, 3), u.cols))
        q = pos[axis(u, 0)]

        def total(j):
            return mine1(u, u.cols, q, j) + r1[u.a][1, j, :, u.cols].astype(F32) + r1[u.a][2, j, :, u.cols].astype(F32)

        if u.a == 1:
            for j in range(4):
                t = total(j)
                for z in range(4):
                    a1[1][z, 12 * j : 12 * j + 12, u.cols] = t[12 * z : 12 * z + 12]
        else:

            @pl.loop(0, 4)
            def _(j):
                a1[u.a][j, :, u.cols] = total(j)

        give(u, 1, 0)
        give(u, 1, 1)

    def st4(u):
        take_in(u, 1, 0)
        give(u, 1, 2)

    def st5(u):
        got(u, 4, view(r2[u.a], 1, slice(1, 3), u.cols))
        rc = RC[u.a]
        t = a1[u.a][pos[axis(u, 1)], :, u.cols] + r2[u.a][1, :, u.cols].astype(F32) + r2[u.a][2, :, u.cols].astype(F32)
        for q in range(4):
            a2[u.a][q, 0:rc, u.cols] = t[rc * q : rc * q + rc]
        give_all(u)

    def st6(u):
        got(u, 6, r3[u.a].at[:, :, u.cols])
        h, rp = H[u.a], RP[u.a]
        t = a2[u.a][pos[axis(u, 2)], :, u.cols]
        for n in range(3):
            t = t + r3[u.a][n, :, u.cols].astype(F32)
        for q in range(2):
            grad = t[h * q : h * q + h].astype(BF).astype(F32)
            new, mn, vn = adamw(wsel[u.a][q, 0:h, u.cols], msel[u.a][q, 0:h, u.cols], vsel[u.a][q, 0:h, u.cols], grad)
            tmp[h * q : h * q + h, 0 : u.cn] = new
            ms[u.a][q, 0:h, u.cols] = mn
            vs[u.a][q, 0:h, u.cols] = vn
        ag3[u.a][pos[axis(u, 2)], :, u.cols] = tmp[0:rp, 0 : u.cn].astype(BF)
        block = ag3[u.a].at[pos[axis(u, 2)], :, u.cols]
        post(u, 7, [(block, block, near(axis(u, 2), d)) for d in (2, 1, -1)], ag3[u.a].at[0:3, :, u.cols])
        pairs_of = [(x[u.a].at[1 - c, :, u.cols], y[u.a].at[c, :, u.cols], partner) for x, y in ((ms, mo), (vs, vo))]
        post(u, 15, pairs_of, ms[u.a].at[:, :, u.cols])
        for x, y in ((ms, mo), (vs, vo)):
            y[u.a][c, 0:h, u.cols] = x[u.a][c, 0:h, u.cols]

    def ref2(u, cols):
        if u.a == 0:
            return lambda q: out[0].at[c, pos[0], q, :, cols]
        if u.a == 1:
            return lambda q: ag2u.at[q, :, cols]
        return lambda q: out[2].at[c, pos[2], q, :, cols]

    def ref1(u, cols, layer=c):
        if u.a == 1:
            return lambda q: out[1].at[layer, :, q, :, cols]
        return lambda q: out[u.a].at[layer, q, :, :, cols]

    refs_of = (ref1, ref2)

    def base(phase):
        return 11 - 3 * phase

    def spread(u, phase, i):
        sends = []
        for t in u.units:
            block = refs_of[phase](u, t.cols)(at(u, phase, -t.s) if i == 2 else pos[axis(u, phase)])
            sends.append((block, block, near(axis(u, phase), -t.s if i == 1 else t.s)))
        post(u, base(phase) + i, sends, thrice(u, phase))

    def arrived(u, phase, i):
        got(u, base(phase) + i, refs_of[phase](u, u.cols)(at(u, phase, 2)))

    def thrice(u, phase):
        return out[u.a].at[c, 0:3, :, :, u.cols] if phase == 0 else out[u.a].at[c, 0, 0:3, :, u.cols]

    def over(u, d):
        if d % 2 == 0:
            block = ref1(u, u.cols)(at(u, 0, d))
            sends = [(block, block, partner)]
        else:
            blocks = [ref1(u, t.cols)(at(u, 0, d * t.s)) for t in u.units]
            sends = [(x, x, partner) for x in blocks]
        post(u, 16, sends, out[u.a].at[c, :, :, :, u.cols])

    def st7(u):
        got(u, 7, ag3[u.a].at[0:3, :, u.cols])
        rc, r = RC[u.a], R[u.a]
        for q in range(4):
            tmp[rc * q : rc * q + rc, 0 : u.cn] = ag3[u.a][q, 0:rc, u.cols].astype(F32)
        ref2(u, u.cols)(pos[axis(u, 1)])[...] = tmp[0:r, 0 : u.cn].astype(BF)
        spread(u, 1, 0)
        spread(u, 1, 1)

    def st8(u):
        arrived(u, 1, 0)
        spread(u, 1, 2)

    def st9(u):
        got(u, 9, out[u.a].at[c, 0, 0:2, :, u.cols])
        if u.a == 1:
            for x in range(4):
                for z in range(4):
                    tmp[12 * z : 12 * z + 12, 0 : u.cn] = ag2u[z, 12 * x : 12 * x + 12, u.cols].astype(F32)
                out[1][c, x, pos[1], :, u.cols] = tmp[0:48, 0 : u.cn].astype(BF)
        spread(u, 0, 0)

    def st10(u):
        spread(u, 0, 1)

    def st11(u):
        over(u, 0)

    def st12(u):
        arrived(u, 0, 0)
        spread(u, 0, 2)

    def st13(u):
        over(u, -1)

    def st14(u):
        arrived(u, 0, 1)
        over(u, 1)

    def st15(u):
        arrived(u, 0, 2)
        over(u, 2)

    def st16(u):
        got(u, 15, mo[u.a].at[:, :, u.cols])
        got(u, 16, out[u.a].at[1 - c, :, :, :, u.cols])

    small, swaps = [], []
    for a in range(3):
        small.append((wh[a].at[c, pos[0], pos[1]], wz[a]))
        small.append((mh[a], m[a]))
        small.append((vh[a], v[a]))
        swaps.append((mh[a], pm[a]))
        swaps.append((vh[a], pv[a]))
    small = [pltpu.make_async_copy(src, dst, msem.at[n]) for n, (src, dst) in enumerate(small)]
    swaps = [
        pltpu.make_async_remote_copy(
            src_ref=src, dst_ref=dst, send_sem=psem.at[n], recv_sem=qsem.at[n], device_id=(rep, partner), device_id_type=MESH
        )
        for n, (src, dst) in enumerate(swaps)
    ]

    def prepare():
        for one in small:
            one.wait()
        for one in swaps:
            one.wait()
        for a in range(3):
            h = H[a]
            for src, theirs, dst in ((m, pm, msel), (v, pv, vsel)):
                dst[a][c, 0:h] = jnp.where(c == 0, src[a][:, 0], src[a][:, 1])
                dst[a][1 - c, 0:h] = jnp.where(c == 0, theirs[a][:, 0], theirs[a][:, 1])

            @pl.loop(0, COLS[a] // 256)
            def _(j):
                cols = pl.ds(pl.multiple_of(j * 256, 256), 256)
                line = wz[a][:, cols].astype(F32)
                for q in range(2):
                    rows = line[h * q : h * q + h]
                    for z in range(1, 4):
                        rows = jnp.where(pos[2] == z, line[h * (2 * z + q) : h * (2 * z + q) + h], rows)
                    wsel[a][q, 0:h, cols] = rows

    by_chunk = sorted(all_pairs, key=lambda u: ((u.chunk + 1) / len(TILES[u.a]), u.p))
    for u in by_chunk:
        loads(u).start()
    barrier = pltpu.get_barrier_semaphore()
    peers = [partner] + [near(x, d) for x in range(3) for d in (1, -1, 2)]
    for peer in peers:
        pl.semaphore_signal(barrier, inc=1, device_id=(rep, peer), device_id_type=MESH)
    pl.semaphore_wait(barrier, len(peers))

    for n, u in enumerate(by_chunk):
        swap(u)
        if n == FIRST:
            for one in swaps:
                one.start()
            for one in small:
                one.start()

    stages = (st0, st1, st2, st3, st4, st5, st6, st7, st8, st9, st10, st11, st12, st13, st14, st15, st16)
    done = [0] * len(all_pairs)
    for n, letter in enumerate("".join(ORDER)):
        p = ord(letter) - ord("a")
        stages[done[p]](all_pairs[p])
        done[p] += 1
        if n == PREPARE:
            prepare()
    for _, wait in leaving.values():
        wait()


def finish_kernel(*refs):
    it = iter(refs)

    def take(n):
        return [next(it) for _ in range(n)]

    src, moments, out, new = take(3), take(6), take(3), take(6)
    buf, tmp, sem, bsem = take(4)
    turned = take(6)
    copies = [pltpu.make_async_copy(x, y, sem.at[i]) for i, (x, y) in enumerate(zip(src[:2] + turned, out[:2] + new, strict=True))]
    for one in copies[:2]:
        one.start()
    for n in range(6):
        for layer in range(2):
            turned[n][:, layer] = moments[n][layer, 0 : H[n % 3]]
        copies[2 + n].start()

    def back(layer, x, n):
        return pltpu.make_async_copy(buf.at[n], out[2].at[layer, x], bsem.at[n])

    for layer in range(2):
        for x in range(4):
            n = 4 * layer + x

            @pl.loop(0, 3)
            def _(j):
                cols = pl.ds(pl.multiple_of(j * 256, 256), 256)
                for y in range(4):
                    for z in range(4):
                        tmp[28 * z : 28 * z + 28] = src[2][layer, z, x, 28 * y : 28 * y + 28, cols].astype(F32)
                    buf[n, y, :, cols] = tmp[...].astype(BF)

            back(layer, x, n).start()
    for layer in range(2):
        for x in range(4):
            back(layer, x, 4 * layer + x).wait()
    for one in copies:
        one.wait()


def solution(mesh):
    def step(*arrays):
        terms, weights, m, v = (arrays[i : i + 3] for i in (0, 3, 6, 9))
        whole = [(2, 4, 4, R[a], COLS[a]) for a in range(3)]
        terms = [t[0].reshape(s) for t, s in zip(terms, whole, strict=True)]
        views = [w.reshape(s) for w, s in zip(weights, whole, strict=True)]
        m, v = ([x.transpose(1, 0, 2) for x in y] for y in (m, v))
        vmem = pl.BlockSpec(memory_space=pltpu.VMEM)
        hbm = pl.BlockSpec(memory_space=pl.ANY)
        per = lambda fn, dt: [pltpu.VMEM(fn(a), dt) for a in range(3)]
        moment = lambda a: (H[a], 2, COLS[a])
        rows = lambda a: (2, 8 if a < 2 else 16, COLS[a])
        n = len(pairs())
        scratch = (
            per(lambda a: (4, 4, R[a], COLS[a]), BF) * 2
            + [pltpu.VMEM((4, 4, R[2], COLS[2]), F32)]
            + per(lambda a: (3, 4, R[a], COLS[a]), BF) * 2
            + per(lambda a: (4, R[a], COLS[a]), F32)
            + per(lambda a: (3, R[a], COLS[a]), BF) * 2
            + per(lambda a: (4, RP[a], COLS[a]), F32)
            + per(lambda a: (3, RP[a], COLS[a]), BF) * 2
            + per(lambda a: (4, RP[a], COLS[a]), BF)
            + per(lambda a: (R[a], COLS[a]), BF)
            + per(rows, F32) * 5
            + per(moment, F32) * 4
            + [pltpu.VMEM((4, 48, COLS[1]), BF), pltpu.VMEM((112, 256 * max(max(t) for t in TILES)), F32)]
            + [pltpu.SemaphoreType.DMA((k,)) for k in (n, 9, 6, 6)]
            + [pltpu.SemaphoreType.DMA((n, max(SEND) + 1)), pltpu.SemaphoreType.DMA((n, max(RECV) + 1))]
        )
        got = pl.pallas_call(
            comm_kernel,
            out_shape=[pltpu.VMEM(s, BF) for s in whole] + per(rows, F32) * 2,
            in_specs=[hbm] * 12,
            out_specs=[vmem] * 9,
            scratch_shapes=scratch,
            compiler_params=pltpu.CompilerParams(collective_id=0, has_side_effects=True, vmem_limit_bytes=VMEM_LIMIT),
        )(*terms, *views, *m, *v)
        kept = [pltpu.with_memory_space_constraint(x, pltpu.VMEM) for x in got]
        done = pl.pallas_call(
            finish_kernel,
            out_shape=[jax.ShapeDtypeStruct(s, BF) for s in whole] + [jax.ShapeDtypeStruct(moment(a), F32) for a in range(3)] * 2,
            in_specs=[vmem] * 9,
            out_specs=[hbm] * 9,
            scratch_shapes=[
                pltpu.VMEM((8, 4, R[2], COLS[2]), BF),
                pltpu.VMEM((112, 256), F32),
                pltpu.SemaphoreType.DMA((8,)),
                pltpu.SemaphoreType.DMA((8,)),
            ]
            + per(moment, F32) * 2,
            compiler_params=pltpu.CompilerParams(vmem_limit_bytes=20_000_000),
        )(*kept)
        return [x.reshape(w.shape) for x, w in zip(done[:3], weights, strict=True)] + [x.transpose(1, 0, 2) for x in done[3:]]

    def run(*arrays):
        return tuple(step(*arrays))

    all_of, cut = P(None, None, None), P(None, "dp", None)
    return jax.shard_map(
        run,
        mesh=mesh,
        in_specs=(P(("rep", "dp"), None, None, None),) * 3 + (all_of,) * 3 + (cut,) * 6,
        out_specs=(P("rep", None, None),) * 3 + (P("rep", "dp", None),) * 6,
        check_vma=False,
    )
```
